256 devices in a mesh: grp: 4 (over y), cp: 64 (over x, z, core).
Axes of the slice: x: 4, y: 4, z: 8, core: 2. Of those that a mesh axis runs over, the one named last changes fastest.
Arguments:
- queries: bfloat16 [131072, 2048], P(('grp', 'cp')), parts along dimension 0, may hold values from -6 to 6
- keys: bfloat16 [131072, 1024], P(('grp', 'cp')), parts along dimension 0, may hold values from -8 to 8
- values: bfloat16 [131072, 1024], P(('grp', 'cp')), parts along dimension 0, may hold values from -6 to 6
- doc_lengths: int32 [1024], P('grp'), parts along dimension 0, may hold values from 1 to 1024, 32768 in all
Outputs:
- attended: bfloat16 [131072, 2048], P(('grp', 'cp')), parts along dimension 0
The draws below stay inside these ranges and needn't reach their ends.
There are 4 independent parts, one for each index of `grp`. The reference program is written for one: setup_inputs(seed, part) draws one part's arguments, and reference() takes and returns one part's arrays. A program takes and returns all parts, laid end to end along the dimension named above; each array names one. Nothing has to cross between parts.
Inputs may be any that keep to these rules, and one draw needn't show every extreme that they name: doc_lengths sums to 32768, and its largest entry is exactly 1024.
All inputs are finite; a program needn't handle non-finite values.
Results may differ from the reference program's by a relative error of at most 0.0031.
Values may be sent and summed in bfloat16 or wider, within the bound.
A program may use at most 64 MiB of HBM per device.

```python
import math
import jax
import jax.numpy as jnp
import numpy as np
from jax import lax

HQ = 16
HK = 8
DH = 128
TOK_DEV = 512
REACH = 2
TOKENS = 32768
MAXDOC = 1024
DOCS = 256


def draw_queries(key, part):
    drawn = jnp.clip(jax.random.normal(jax.random.fold_in(key, 11), (TOKENS, HQ * DH), jnp.float32), -6.0, 6.0)
    return drawn.astype(jnp.bfloat16)


def draw_keys(key, part):
    drawn = jnp.clip(jax.random.normal(jax.random.fold_in(key, 22), (TOKENS, HK * DH), jnp.float32), -6.0, 6.0)
    return drawn.astype(jnp.bfloat16)


def shard_levels(rng, extent, shards, low, largest):
    factor_of, own = 1.0, jax.random.fold_in(rng, 6)
    for dim, blocks in shards:
        draws = jnp.exp(jax.random.uniform(jax.random.fold_in(own, dim), (blocks,), jnp.float32, low / len(shards), largest / len(shards)))
        factor_of = factor_of * jnp.repeat(draws, extent[dim] // blocks).reshape([-1 if axis == dim else 1 for axis in range(len(extent))])
    return factor_of


def profile(count, total, bound, skew):
    weights = [(1 << 20) // math.isqrt(standing ** skew) + 1 for standing in range(2, count + 1)]
    surplus, given = total - bound - (count - 1), [1] * (count - 1)
    while surplus > 0:
        movable = [i for i in range(count - 1) if given[i] < bound]
        mass, remaining = sum([weights[i] for i in movable]), surplus
        for i in movable:
            extra = min(bound - given[i], max(1, remaining * weights[i] // mass), surplus)
            given[i] = given[i] + extra
            surplus = surplus - extra
    return np.array([bound] + given)


def ragged_sizes(key, number_of, total, most, skew):
    if number_of == 2:
        one = jax.random.randint(key, (), max(1, total - most), min(most, total - 1) + 1)
        return jnp.stack([one, total - one])
    lengths = jnp.asarray(profile(number_of, total, most, skew), jnp.int32)
    couples = (number_of - 1) // 2
    source_of, taker = lengths[1:1 + 2 * couples:2], lengths[2:2 + 2 * couples:2]
    room = jnp.minimum(source_of - 1, most - taker)
    passed = jax.random.randint(jax.random.fold_in(key, 1), (couples,), 0, 1 << 20) % (room + 1)
    lengths = lengths.at[1:1 + 2 * couples:2].set(source_of - passed).at[2:2 + 2 * couples:2].set(taker + passed)
    return lengths[jax.random.permutation(jax.random.fold_in(key, 2), number_of)]


def noise(rng, dims, spread, limit, shards=(), held_as=jnp.bfloat16):
    loudness = shard_levels(rng, dims, shards, -0.22, 0.18) if shards else 1.0
    array = jax.random.normal(rng, dims, jnp.float32) * spread * loudness
    return jnp.minimum(jnp.maximum(array, -limit), limit).astype(held_as)


def setup_inputs(seed: int = 0, part: int = 0) -> dict:
    arg_keys = jax.random.split(jax.random.key(seed), 5)
    part_splits = jax.random.split(jax.random.fold_in(arg_keys[4], part), 5)
    queries = draw_queries(jax.random.fold_in(jax.random.fold_in(arg_keys[4], part), 71), part)
    keys = draw_keys(jax.random.fold_in(jax.random.fold_in(arg_keys[4], part), 71), part)
    values = noise(part_splits[2], (TOKENS, HK * DH), 1.0, 6.0, ((0, 64),))
    doc_lengths = ragged_sizes(part_splits[3], DOCS, TOKENS, MAXDOC, 2).astype(jnp.int32)
    return {"queries": queries, "keys": keys, "values": values, "doc_lengths": doc_lengths}


query_scale = 144.0 ** -0.5


def doc_index(positions, doc_ends):
    return jnp.sum((positions[:, None] >= doc_ends[None, :]).astype(jnp.int32), axis=1).astype(jnp.int32)


def attend(query_rows, key_rows, value_rows, visible):
    tok_rows = query_rows.shape[0]
    key_count = key_rows.shape[0]
    groups = HQ // HK
    query_heads = query_rows.astype(jnp.float32).reshape(tok_rows, HK, groups, DH)
    key_heads = key_rows.astype(jnp.float32).reshape(key_count, HK, DH)
    value_heads = value_rows.astype(jnp.float32).reshape(key_count, HK, DH)
    scores = jnp.einsum("tkgd,wkd->kgtw", query_heads, key_heads) * query_scale
    scores = jnp.where(visible[None, None], scores, -jnp.inf)
    highest = jnp.max(scores, axis=-1, keepdims=True)
    weights = jnp.exp(scores - highest)
    totals = jnp.sum(weights, axis=-1)
    rounded = lax.optimization_barrier(weights.astype(jnp.bfloat16))
    mixed = jnp.einsum("kgtw,wkd->tkgd", rounded.astype(jnp.float32), value_heads)
    mixed = mixed / jnp.transpose(totals, (2, 0, 1))[..., None]
    return mixed.reshape(tok_rows, HQ * DH).astype(jnp.bfloat16)


def reference(queries, keys, values, doc_lengths):
    doc_ends = jnp.cumsum(doc_lengths).astype(jnp.int32)
    margin = REACH * TOK_DEV
    window = (REACH + 1) * TOK_DEV
    pad_keys = jnp.concatenate([jnp.zeros((margin, HK * DH), keys.dtype), keys], axis=0)
    pad_values = jnp.concatenate([jnp.zeros((margin, HK * DH), values.dtype), values], axis=0)

    def one_block(index):
        begin_row = (index * TOK_DEV).astype(jnp.int32)
        query_pos = begin_row + jnp.arange(TOK_DEV, dtype=jnp.int32)
        key_pos = begin_row - margin + jnp.arange(window, dtype=jnp.int32)
        same_doc = doc_index(query_pos, doc_ends)[:, None] == doc_index(key_pos, doc_ends)[None, :]
        visible = same_doc & (key_pos[None, :] <= query_pos[:, None]) & (key_pos[None, :] >= 0)
        query_rows = lax.dynamic_slice_in_dim(queries, begin_row, TOK_DEV, 0)
        key_rows = lax.dynamic_slice_in_dim(pad_keys, begin_row, window, 0)
        value_rows = lax.dynamic_slice_in_dim(pad_values, begin_row, window, 0)
        return attend(query_rows, key_rows, value_rows, visible)

    blocks = lax.map(one_block, jnp.arange(TOKENS // TOK_DEV, dtype=jnp.int32))
    return blocks.reshape(TOKENS, HQ * DH)
```

```python
import functools
import math

import jax
import jax.numpy as jnp
from jax import lax
from jax.experimental import pallas as pl
from jax.experimental.pallas import tpu as pltpu
from jax.sharding import PartitionSpec as P

HQ = 16
HK = 8
DH = 128
REACH = 2
GROUPS = HQ // HK
WIDTH = GROUPS * DH
TILE = 128
MASKED = -1e30

exponent_scale = 144.0 ** (-0.5) * math.log2(math.e)


LOG2E = math.log2(math.e)
SPLIT = HK // 2
MODULUS = 63
APART = 65536.0
SCORE_KEYS = 640
MIX_KEYS = 256
MIX_STEP = 64
MESH = pl.DeviceIdType.MESH


def kernel(
    shards,
    lengths_ref,
    queries_ref,
    keys_ref,
    values_ref,
    out_ref,
    held,
    query_held,
    out_held,
    query_back,
    slot,
    stat_out,
    stat_in,
    turned,
    key_marks,
    query_marks,
    scores,
    load_sem,
    query_sem,
    out_sem,
    core_send,
    core_recv,
    query_send,
    query_recv,
    slot_send,
    slot_recv,
    relay_send,
    relay_recv,
    stat_send,
    stat_recv,
):
    me = lax.axis_index("cp")
    core = lax.rem(me, 2)
    even = core == 0
    odd = core == 1
    partner = me + 1 - 2 * core
    rows = keys_ref.shape[0]
    docs = lengths_ref.shape[0]
    tiles = rows // TILE
    window = REACH * rows + TILE
    own = pl.ds(REACH * rows, rows)
    near = pl.ds(rows, rows)
    far = pl.ds(0, rows)
    has_prev = me >= 2
    has_next = me < shards - 2
    chip_begin = (me - core) * rows
    next_begin = chip_begin + 2 * rows

    def loads(head):
        lanes = pl.ds(pl.multiple_of(head * DH, DH), DH)
        return (
            pltpu.make_async_copy(keys_ref.at[:, lanes], held.at[head, 0, own], load_sem.at[head, 0]),
            pltpu.make_async_copy(values_ref.at[:, lanes], held.at[head, 1, own], load_sem.at[head, 1]),
        )

    def query_load(head):
        lanes = pl.ds(pl.multiple_of(head * WIDTH, WIDTH), WIDTH)
        return pltpu.make_async_copy(queries_ref.at[:, lanes], query_held.at[head], query_sem.at[head])

    def out_store(head):
        lanes = pl.ds(pl.multiple_of(head * WIDTH, WIDTH), WIDTH)
        return pltpu.make_async_copy(out_held.at[head], out_ref.at[:, lanes], out_sem.at[head])

    def remote(source, target, send, recv, device):
        return pltpu.make_async_remote_copy(
            src_ref=source,
            dst_ref=target,
            send_sem=send,
            recv_sem=recv,
            device_id={"cp": device},
            device_id_type=MESH,
        )

    def to_core(head, region):
        return remote(
            held.at[head, :, own], held.at[head, :, region], core_send.at[head], core_recv.at[head], partner
        )

    def query_to_prev(step, side):
        return remote(
            query_held.at[side * SPLIT + step],
            query_back.at[step],
            query_send.at[side * SPLIT + step],
            query_recv.at[step],
            me - 2 + side,
        )

    def slot_to_next(step, region):
        return remote(
            slot.at[step],
            held.at[core * SPLIT + step, :, region],
            slot_send.at[step],
            slot_recv.at[step],
            me + 2,
        )

    def relay(step, source, target):
        head = core * SPLIT + step
        return remote(
            held.at[head, :, source], held.at[head, :, target], relay_send.at[step], relay_recv.at[step], partner
        )

    def stat_to_next(step, head):
        return remote(
            stat_out.at[step], stat_in.at[head], stat_send.at[step], stat_recv.at[head], me + 2 - core
        )

    @pl.loop(0, SPLIT)
    def _(step):
        query_load(step).start()
        query_load(SPLIT + step).start()

    @pl.loop(0, HK)
    def _(head):
        for copy in loads(head):
            copy.start()

    barrier = pltpu.get_barrier_semaphore()

    def greet(device):
        pl.semaphore_signal(barrier, inc=1, device_id={"cp": device}, device_id_type=MESH)

    greet(partner)

    @pl.when(has_prev)
    def _():
        greet(me - 2)

        @pl.when(even)
        def _():
            greet(me - 1)

    @pl.when(has_next)
    def _():
        greet(me + 2)

        @pl.when(odd)
        def _():
            greet(me + 1)

    back_peers = jnp.where(has_prev, 2 - core, 0)
    next_peers = jnp.where(has_next, 1 + core, 0)
    pl.semaphore_wait(barrier, 1 + back_peers + next_peers)

    @pl.loop(0, SPLIT)
    def _(step):
        for side in range(2):
            query_load(side * SPLIT + step).wait()

            @pl.when(jnp.logical_and(even, has_prev))
            def _():
                query_to_prev(step, side).start()

    @pl.loop(0, HK)
    def _(head):
        for copy in loads(head):
            copy.wait()

        @pl.when(even)
        def _():
            to_core(head, near).start()

        @pl.when(jnp.logical_and(odd, head < SPLIT))
        def _():
            to_core(head, far).start()

    @pl.when(jnp.logical_not(has_prev))
    def _():
        @pl.when(even)
        def _():
            held[:, :, near, :] = jnp.zeros((HK, 2, rows, DH), held.dtype)
            stat_in[...] = jnp.full(stat_in.shape, MASKED, jnp.float32)

        @pl.when(odd)
        def _():
            held[:, :, far, :] = jnp.zeros((HK, 2, rows, DH), held.dtype)

    row = lax.broadcasted_iota(jnp.int32, (4 * tiles, TILE), 0)
    lane = lax.broadcasted_iota(jnp.int32, (4 * tiles, TILE), 1)
    far_begin = jnp.where(even, me + 1, me - 2) * rows
    region_begin = jnp.where(
        row < tiles,
        far_begin,
        jnp.where(
            row < 2 * tiles,
            (me - 1) * rows - rows,
            jnp.where(row < 3 * tiles, me * rows - 2 * rows, next_begin - 3 * rows),
        ),
    )
    positions = region_begin + row * TILE + lane
    edge_row = lax.broadcasted_iota(jnp.int32, (8, TILE), 0)
    edges = jnp.where(edge_row == 0, chip_begin, next_begin)

    def next_docs(step, state):
        end, doc, begins = state
        for k in range(8):
            end = end + lengths_ref[step * 8 + k]
            doc = doc + (positions >= end).astype(jnp.int32)
            begins = jnp.where(edges >= end, end, begins)
        return end, doc, begins

    _, doc, begins = lax.fori_loop(
        0,
        docs // 8,
        next_docs,
        (jnp.int32(0), jnp.zeros(positions.shape, jnp.int32), jnp.zeros(edges.shape, jnp.int32)),
    )
    sends_keys = (edges - begins <= rows).astype(jnp.int32)
    next_keys = jnp.broadcast_to(sends_keys[1:2, :], (TILE, DH)) > 0
    prev_keys = jnp.broadcast_to(sends_keys[0:1, :], positions.shape)
    prev_row = jnp.where(even, 1, 0)
    from_prev = (row >= prev_row * tiles) & (row < (prev_row + 1) * tiles)
    none = (positions < 0) | (from_prev & (prev_keys == 0))
    rest = doc
    for k in range(1, docs // MODULUS + 1):
        rest = rest - jnp.where(doc >= k * MODULUS, MODULUS, 0)
    code_low = jnp.where(none, 2 * DH, doc & (DH // 2 - 1))
    code_high = jnp.where(none, 2 * DH, rest + DH // 2)
    feature = lax.broadcasted_iota(jnp.int32, (DH, TILE), 0)

    def matches(block):
        return (feature == code_low[block : block + 1, :]) | (feature == code_high[block : block + 1, :])

    for block in range(3 * tiles):
        missing = jnp.where(matches(block), 0.0, -APART).astype(jnp.bfloat16)
        key_marks[pl.ds(block * TILE, TILE), :] = missing.T
    for block in range(2 * tiles):
        present = jnp.where(matches(2 * tiles + block), 1.0, 0.0).astype(jnp.bfloat16)
        query_marks[:, pl.ds(block * TILE, TILE)] = present

    causal = lax.broadcasted_iota(jnp.int32, (TILE, WIDTH), 0) <= lax.rem(
        lax.broadcasted_iota(jnp.int32, (TILE, WIDTH), 1), TILE
    )

    def turn_values(head, region):
        for tile in range(tiles):
            span = pl.ds(region + tile * TILE, TILE)
            turned[head, :, span] = held[head, 1, span, :].T

    def pieces(spans, size):
        cut, at = [], 0
        for begin, count in spans:
            done = 0
            while done < count:
                step = min(size, count - done)
                cut.append((begin + done, at, step))
                done, at = done + step, at + step
        return cut

    def score_job(job, buffer):
        head, queries, marks, spans, own_end, _ = job
        state = {"highest": None, "buffer": buffer}
        turned_queries = jnp.concatenate([queries[:, g * DH : (g + 1) * DH].T for g in range(GROUPS)], axis=1)
        right = jnp.concatenate([turned_queries, jnp.concatenate([marks] * GROUPS, axis=1)], axis=0)
        total = sum(count for _, count in spans)

        def piece(begin, at, count):
            span = pl.ds(begin, count)
            left = jnp.concatenate([held[head, 0, span, :], key_marks[span, :]], axis=1)
            part = jnp.dot(left, right, preferred_element_type=jnp.float32)
            if own_end and at + count == total:
                last = jnp.where(causal, part[count - TILE :], -APART)
                part = jnp.concatenate([part[: count - TILE], last], axis=0) if count > TILE else last
            scores[buffer, pl.ds(at, count), :] = part
            top = jnp.max(part.reshape(count // 8, 8, WIDTH), axis=0)
            state["highest"] = top if state["highest"] is None else jnp.maximum(state["highest"], top)

        def finish():
            state["row"] = jnp.max(state["highest"], axis=0, keepdims=True)

        return state, [functools.partial(piece, *cut) for cut in pieces(spans, SCORE_KEYS)], finish

    def mix_job(job, state):
        head, _, _, spans, _, store = job
        buffer, highest = state["buffer"], state["row"]
        sums = {"totals": None, "mixed": None}

        def piece(begin, at, count):
            span = pl.ds(begin, count)
            rounded = []
            for sub in range(0, count, MIX_STEP):
                part = scores[buffer, pl.ds(at + sub, MIX_STEP), :]
                weights = jnp.exp2((part - highest) * exponent_scale)
                total = jnp.sum(weights.reshape(MIX_STEP // 8, 8, WIDTH), axis=0)
                sums["totals"] = total if sums["totals"] is None else sums["totals"] + total
                rounded.append(weights.astype(jnp.bfloat16))
            mixed = jnp.dot(
                turned[head, :, span], jnp.concatenate(rounded, axis=0), preferred_element_type=jnp.float32
            )
            sums["mixed"] = mixed if sums["mixed"] is None else sums["mixed"] + mixed

        def finish():
            totals = jnp.sum(sums["totals"], axis=0, keepdims=True)
            store(highest * exponent_scale, totals, sums["mixed"])

        return [functools.partial(piece, *cut) for cut in pieces(spans, MIX_KEYS)], finish

    def run(jobs):
        before = None
        for index, job in enumerate(jobs + [None]):
            state, score, score_end, mix, mix_end = None, [], None, [], None
            if job is not None:
                state, score, score_end = score_job(job, index % scores.shape[0])
            if before is not None:
                mix, mix_end = mix_job(*before)
            for step in range(max(len(score), len(mix))):
                if step < len(score):
                    score[step]()
                if step < len(mix):
                    mix[step]()
            if mix_end is not None:
                mix_end()
            if score_end is not None:
                score_end()
            before = (job, state)

    def attend_back(head, step, older, newer):
        jobs = []
        for tile in range(tiles):
            span = pl.ds(tile * TILE, TILE)

            def store(level, totals, mixed, tile=tile, span=span):
                mixed = (mixed * (1.0 / totals)).astype(jnp.bfloat16)
                level = level + jnp.log(totals) * LOG2E
                sent = pl.ds(newer + tile * TILE, TILE)
                for g in range(GROUPS):
                    part = pl.ds(g * DH, DH)
                    turned_back = mixed[:, g * DH : (g + 1) * DH].T
                    slot[step, g, span, :] = jnp.where(next_keys, held[head, g, sent, :], turned_back)
                    stat_out[step, pl.ds(tile * GROUPS + g, 1), :] = jnp.where(
                        next_keys[:1, :], MASKED, level[:, g * DH : (g + 1) * DH]
                    )

            spans = [(older + tile * TILE, rows - tile * TILE), (newer, rows)]
            marks = query_marks[:, pl.ds(rows + tile * TILE, TILE)]
            jobs.append((head, query_back[step, span, :], marks, spans, False, store))
        run(jobs)

    def put(head, span, mixed):
        for g in range(GROUPS):
            out_held[head, span, pl.ds(g * DH, DH)] = mixed[:, g * DH : (g + 1) * DH].T

    def attend_even(head):
        jobs = []
        for tile in range(tiles):
            span = pl.ds(tile * TILE, TILE)

            def store(level, totals, mixed, tile=tile, span=span):
                sent = pl.ds(rows + tile * TILE, TILE)
                other = jnp.concatenate(
                    [stat_in[head, pl.ds(tile * GROUPS + g, 1), :] for g in range(GROUPS)], axis=1
                )
                top = jnp.maximum(level, other)
                here = jnp.exp2(level - top)
                there = jnp.exp2(other - top)
                share = 1.0 / (totals * here + there)
                partial = jnp.concatenate([held[head, 0, sent, :].T, turned[head, :, sent]], axis=1)
                both = mixed * (here * share) + partial.astype(jnp.float32) * (there * share)
                put(head, span, both.astype(jnp.bfloat16))

            spans = [(rows, rows + (tile + 1) * TILE)]
            marks = query_marks[:, span]
            jobs.append((head, query_held[head, span, :], marks, spans, True, store))
        run(jobs)

    def attend_odd(head):
        jobs = []
        for tile in range(tiles):
            span = pl.ds(tile * TILE, TILE)

            def store(level, totals, mixed, span=span):
                put(head, span, (mixed * (1.0 / totals)).astype(jnp.bfloat16))

            spans = [(tile * TILE, REACH * rows + TILE)]
            marks = query_marks[:, span]
            jobs.append((head, query_held[head, span, :], marks, spans, True, store))
        run(jobs)

    @pl.loop(0, HK)
    def _(head):
        turn_values(head, REACH * rows)

    @pl.when(even)
    def _():
        @pl.loop(0, SPLIT)
        def _(head):
            to_core(head, far).wait_recv()
            turn_values(head, 0)

    @pl.when(odd)
    def _():
        @pl.loop(0, HK)
        def _(head):
            to_core(head, near).wait_recv()
            turn_values(head, rows)

    @pl.loop(0, SPLIT + 1)
    def _(turn):
        @pl.when(jnp.logical_and(has_next, turn < SPLIT))
        def _():
            query_to_prev(turn, 0).wait_recv()

            @pl.when(even)
            def _():
                attend_back(turn, turn, 2 * rows, 0)
                slot_to_next(turn, near).start()

            @pl.when(odd)
            def _():
                attend_back(SPLIT + turn, turn, rows, 2 * rows)
                slot_to_next(turn, far).start()

            stat_to_next(turn, core * SPLIT + turn).start()

        @pl.when(turn >= 1)
        def _():
            step = turn - 1

            @pl.when(has_prev)
            def _():
                slot_to_next(step, far).wait_recv()

                @pl.when(even)
                def _():
                    relay(step, near, far).start()

                @pl.when(odd)
                def _():
                    relay(step, far, near).start()

            @pl.loop(0, 2)
            def _(turn_side):
                side = lax.rem(core + turn_side, 2)
                head = side * SPLIT + step

                @pl.when(jnp.logical_and(has_prev, turn_side == 1))
                def _():
                    relay(step, near, far).wait_recv()

                @pl.when(even)
                def _():
                    @pl.when(has_prev)
                    def _():
                        stat_to_next(step, head).wait_recv()

                    turn_values(head, rows)
                    attend_even(head)

                @pl.when(odd)
                def _():
                    turn_values(head, 0)
                    attend_odd(head)

                out_store(head).start()

    @pl.loop(0, HK)
    def _(head):
        out_store(head).wait()

        @pl.when(jnp.logical_or(even, head < SPLIT))
        def _():
            to_core(head, near).wait_send()

    @pl.loop(0, SPLIT)
    def _(step):
        @pl.when(has_next)
        def _():
            slot_to_next(step, near).wait_send()
            stat_to_next(step, step).wait_send()

        @pl.when(has_prev)
        def _():
            relay(step, near, far).wait_send()

            @pl.when(even)
            def _():
                for side in range(2):
                    query_to_prev(step, side).wait_send()


def on_device(queries, keys, values, doc_lengths):
    rows = keys.shape[0]
    shards = lax.axis_size("cp")
    window = REACH * rows + TILE
    stats = rows // TILE * GROUPS
    dma = pltpu.SemaphoreType.DMA
    return pl.pallas_call(
        functools.partial(kernel, shards),
        out_shape=jax.ShapeDtypeStruct(queries.shape, queries.dtype),
        in_specs=[
            pl.BlockSpec(memory_space=pltpu.SMEM),
            pl.BlockSpec(memory_space=pl.ANY),
            pl.BlockSpec(memory_space=pl.ANY),
            pl.BlockSpec(memory_space=pl.ANY),
        ],
        out_specs=pl.BlockSpec(memory_space=pl.ANY),
        scratch_shapes=[
            pltpu.VMEM((HK, 2, (REACH + 1) * rows, DH), keys.dtype),
            pltpu.VMEM((HK, rows, WIDTH), queries.dtype),
            pltpu.VMEM((HK, rows, WIDTH), queries.dtype),
            pltpu.VMEM((SPLIT, rows, WIDTH), queries.dtype),
            pltpu.VMEM((SPLIT, 2, rows, DH), keys.dtype),
            pltpu.VMEM((SPLIT, stats, TILE), jnp.float32),
            pltpu.VMEM((HK, stats, TILE), jnp.float32),
            pltpu.VMEM((HK, DH, (REACH + 1) * rows), keys.dtype),
            pltpu.VMEM(((REACH + 1) * rows, DH), keys.dtype),
            pltpu.VMEM((DH, 2 * rows), keys.dtype),
            pltpu.VMEM((4, window, WIDTH), jnp.float32),
            dma((HK, 2)),
            dma((HK,)),
            dma((HK,)),
            dma((HK,)),
            dma((HK,)),
            dma((HK,)),
            dma((SPLIT,)),
            dma((SPLIT,)),
            dma((SPLIT,)),
            dma((SPLIT,)),
            dma((SPLIT,)),
            dma((SPLIT,)),
            dma((HK,)),
        ],
        compiler_params=pltpu.CompilerParams(
            collective_id=0, has_side_effects=True, vmem_limit_bytes=58 * 1024 * 1024
        ),
    )(doc_lengths, queries, keys, values)


def solution(mesh):
    return jax.shard_map(
        on_device,
        mesh=mesh,
        in_specs=(P(("grp", "cp"), None), P(("grp", "cp"), None), P(("grp", "cp"), None), P("grp")),
        out_specs=P(("grp", "cp"), None),
        check_vma=False,
    )
```

```python
import functools
import math

import jax
import jax.numpy as jnp
from jax import lax
from jax.experimental import pallas as pl
from jax.experimental.pallas import tpu as pltpu
from jax.sharding import PartitionSpec as P

HQ = 16
HK = 8
DH = 128
REACH = 2
GROUPS = HQ // HK
WIDTH = GROUPS * DH
TILE = 128
MASKED = -1e30

exponent_scale = 144.0 ** (-0.5) * math.log2(math.e)


LOG2E = math.log2(math.e)
SPLIT = HK // 2
MODULUS = 63
APART = 65536.0
SCORE_KEYS = 640
MIX_KEYS = 256
MIX_STEP = 64
MESH = pl.DeviceIdType.MESH


def kernel(
    shards,
    lengths_ref,
    queries_ref,
    keys_ref,
    values_ref,
    out_ref,
    held,
    query_held,
    out_held,
    query_back,
    slot,
    stat_out,
    stat_in,
    turned,
    key_marks,
    query_marks,
    scores,
    kept_mix,
    kept_stat,
    load_sem,
    query_sem,
    out_sem,
    core_send,
    core_recv,
    query_send,
    query_recv,
    slot_send,
    slot_recv,
    first_send,
    first_recv,
    relay_send,
    relay_recv,
    stat_send,
    stat_recv,
):
    me = lax.axis_index("cp")
    core = lax.rem(me, 2)
    even = core == 0
    odd = core == 1
    partner = me + 1 - 2 * core
    rows = keys_ref.shape[0]
    docs = lengths_ref.shape[0]
    tiles = rows // TILE
    window = REACH * rows + TILE
    own = pl.ds(REACH * rows, rows)
    near = pl.ds(rows, rows)
    far = pl.ds(0, rows)
    has_prev = me >= 2
    has_next = me < shards - 2
    chip_begin = (me - core) * rows
    next_begin = chip_begin + 2 * rows

    def loads(head):
        lanes = pl.ds(pl.multiple_of(head * DH, DH), DH)
        return (
            pltpu.make_async_copy(keys_ref.at[:, lanes], held.at[head, 0, own], load_sem.at[head, 0]),
            pltpu.make_async_copy(values_ref.at[:, lanes], held.at[head, 1, own], load_sem.at[head, 1]),
        )

    def query_load(head):
        lanes = pl.ds(pl.multiple_of(head * WIDTH, WIDTH), WIDTH)
        return pltpu.make_async_copy(queries_ref.at[:, lanes], query_held.at[head], query_sem.at[head])

    def out_store(head):
        lanes = pl.ds(pl.multiple_of(head * WIDTH, WIDTH), WIDTH)
        return pltpu.make_async_copy(out_held.at[head], out_ref.at[:, lanes], out_sem.at[head])

    def remote(source, target, send, recv, device):
        return pltpu.make_async_remote_copy(
            src_ref=source,
            dst_ref=target,
            send_sem=send,
            recv_sem=recv,
            device_id={"cp": device},
            device_id_type=MESH,
        )

    def to_core(head, region):
        return remote(
            held.at[head, :, own], held.at[head, :, region], core_send.at[head], core_recv.at[head], partner
        )

    def query_to_prev(step, side):
        return remote(
            query_held.at[side * SPLIT + step],
            query_back.at[step],
            query_send.at[side * SPLIT + step],
            query_recv.at[step],
            me - 2 + side,
        )

    def slot_to_next(step, region):
        return remote(
            slot.at[step],
            held.at[core * SPLIT + step, :, region],
            slot_send.at[step],
            slot_recv.at[step],
            me + 2,
        )

    def first_older(side):
        head = side * SPLIT
        return remote(
            held.at[head, :, own], held.at[head, :, far], first_send.at[side], first_recv.at[side], me + 2
        )

    def first_newer(side):
        head = side * SPLIT
        region = far if side else near
        return remote(
            held.at[head, :, own], held.at[head, :, region], first_send.at[side], slot_recv.at[0], me + 1 + side
        )

    def relay(step, source, target):
        head = core * SPLIT + step
        return remote(
            held.at[head, :, source], held.at[head, :, target], relay_send.at[step], relay_recv.at[step], partner
        )

    def stat_to_next(step, head):
        return remote(
            stat_out.at[step], stat_in.at[head], stat_send.at[step], stat_recv.at[head], me + 2 - core
        )

    for side in range(2):
        for copy in loads(side * SPLIT):
            copy.start()

    @pl.loop(1, SPLIT)
    def _(step):
        query_load(step).start()
        query_load(SPLIT + step).start()

    @pl.loop(1, SPLIT)
    def _(step):
        for side in range(2):
            for copy in loads(side * SPLIT + step):
                copy.start()

    query_load(0).start()
    query_load(SPLIT).start()

    barrier = pltpu.get_barrier_semaphore()

    def greet(device):
        pl.semaphore_signal(barrier, inc=1, device_id={"cp": device}, device_id_type=MESH)

    greet(partner)

    @pl.when(has_prev)
    def _():
        greet(me - 2)

        @pl.when(even)
        def _():
            greet(me - 1)

    @pl.when(has_next)
    def _():
        greet(me + 2)

        @pl.when(odd)
        def _():
            greet(me + 1)

    back_peers = jnp.where(has_prev, 2 - core, 0)
    next_peers = jnp.where(has_next, 1 + core, 0)
    pl.semaphore_wait(barrier, 1 + back_peers + next_peers)

    for side in range(2):
        for copy in loads(side * SPLIT):
            copy.wait()

        @pl.when(jnp.logical_and(even, has_next))
        def _():
            first_older(side).start()

        @pl.when(jnp.logical_and(odd, has_next))
        def _():
            first_newer(side).start()

    @pl.loop(1, SPLIT)
    def _(step):
        for side in range(2):
            query_load(side * SPLIT + step).wait()

            @pl.when(jnp.logical_and(even, has_prev))
            def _():
                query_to_prev(step, side).start()

    @pl.when(even)
    def _():
        to_core(0, near).start()
        to_core(SPLIT, near).start()

    @pl.loop(1, SPLIT)
    def _(step):
        for side in range(2):
            head = side * SPLIT + step
            for copy in loads(head):
                copy.wait()

            @pl.when(even)
            def _():
                to_core(head, near).start()

            if side == 0:

                @pl.when(odd)
                def _():
                    to_core(head, far).start()

    query_load(0).wait()
    query_load(SPLIT).wait()

    @pl.when(jnp.logical_not(has_prev))
    def _():
        @pl.when(even)
        def _():
            held[:, :, near, :] = jnp.zeros((HK, 2, rows, DH), held.dtype)
            for side in range(2):
                held[side * SPLIT, :, far, :] = jnp.zeros((2, rows, DH), held.dtype)
            stat_in[...] = jnp.full(stat_in.shape, MASKED, jnp.float32)

        @pl.when(odd)
        def _():
            held[:, :, far, :] = jnp.zeros((HK, 2, rows, DH), held.dtype)

    row = lax.broadcasted_iota(jnp.int32, (6 * tiles, TILE), 0)
    lane = lax.broadcasted_iota(jnp.int32, (6 * tiles, TILE), 1)
    begins_at = jnp.where(
        row < tiles,
        jnp.where(even, me + 1, me - 2) * rows,
        jnp.where(
            row < 3 * tiles,
            (me - 2) * rows,
            jnp.where(row < 4 * tiles, next_begin - 3 * rows, (me - 6) * rows),
        ),
    )
    positions = begins_at + row * TILE + lane
    edge_row = lax.broadcasted_iota(jnp.int32, (8, TILE), 0)
    edges = jnp.where(edge_row == 0, chip_begin, next_begin)

    def next_docs(step, state):
        end, doc, begins = state
        for k in range(8):
            end = end + lengths_ref[step * 8 + k]
            doc = doc + (positions >= end).astype(jnp.int32)
            begins = jnp.where(edges >= end, end, begins)
        return end, doc, begins

    _, doc, begins = lax.fori_loop(
        0,
        docs // 8,
        next_docs,
        (jnp.int32(0), jnp.zeros(positions.shape, jnp.int32), jnp.zeros(edges.shape, jnp.int32)),
    )
    sends_keys = (edges - begins <= rows).astype(jnp.int32)
    next_keys = jnp.broadcast_to(sends_keys[1:2, :], (TILE, DH)) > 0
    prev_keys = jnp.broadcast_to(sends_keys[0:1, :], positions.shape)
    prev_row = jnp.where(even, 1, 0)
    from_prev = (row >= prev_row * tiles) & (row < (prev_row + 1) * tiles)
    none = (positions < 0) | (from_prev & (prev_keys == 0))
    rest = doc
    for k in range(1, docs // MODULUS + 1):
        rest = rest - jnp.where(doc >= k * MODULUS, MODULUS, 0)
    code_low = jnp.where(none, 2 * DH, doc & (DH // 2 - 1))
    code_high = jnp.where(none, 2 * DH, rest + DH // 2)
    feature = lax.broadcasted_iota(jnp.int32, (DH, TILE), 0)

    def matches(block):
        return (feature == code_low[block : block + 1, :]) | (feature == code_high[block : block + 1, :])

    def mark(block):
        return jnp.where(matches(block), 0.0, -APART).astype(jnp.bfloat16).T

    for block in range(2 * tiles):
        key_marks[0, pl.ds(block * TILE, TILE), :] = mark(block)
        key_marks[1, pl.ds(block * TILE, TILE), :] = mark(4 * tiles + block)
    for block in range(2 * tiles, 3 * tiles):
        for kind in range(2):
            key_marks[kind, pl.ds(block * TILE, TILE), :] = mark(block)
    for block in range(2 * tiles):
        present = jnp.where(matches(2 * tiles + block), 1.0, 0.0).astype(jnp.bfloat16)
        query_marks[:, pl.ds(block * TILE, TILE)] = present

    causal = lax.broadcasted_iota(jnp.int32, (TILE, WIDTH), 0) <= lax.rem(
        lax.broadcasted_iota(jnp.int32, (TILE, WIDTH), 1), TILE
    )

    def turn_values(head, region):
        for tile in range(tiles):
            span = pl.ds(region + tile * TILE, TILE)
            turned[head, :, span] = held[head, 1, span, :].T

    def pieces(spans, size):
        cut, at = [], 0
        for begin, count in spans:
            done = 0
            while done < count:
                step = min(size, count - done)
                cut.append((begin + done, at, step))
                done, at = done + step, at + step
        return cut

    def score_job(job, buffer):
        head, queries, marks, kind, spans, own_end, _ = job
        state = {"highest": None, "buffer": buffer}
        turned_queries = jnp.concatenate([queries[:, g * DH : (g + 1) * DH].T for g in range(GROUPS)], axis=1)
        right = jnp.concatenate([turned_queries, jnp.concatenate([marks] * GROUPS, axis=1)], axis=0)
        total = sum(count for _, count in spans)

        def piece(begin, at, count):
            span = pl.ds(begin, count)
            left = jnp.concatenate([held[head, 0, span, :], key_marks[kind, span, :]], axis=1)
            part = jnp.dot(left, right, preferred_element_type=jnp.float32)
            if own_end and at + count == total:
                last = jnp.where(causal, part[count - TILE :], -APART)
                part = jnp.concatenate([part[: count - TILE], last], axis=0) if count > TILE else last
            scores[buffer, pl.ds(at, count), :] = part
            top = jnp.max(part.reshape(count // 8, 8, WIDTH), axis=0)
            state["highest"] = top if state["highest"] is None else jnp.maximum(state["highest"], top)

        def finish():
            state["row"] = jnp.max(state["highest"], axis=0, keepdims=True)

        return state, [functools.partial(piece, *cut) for cut in pieces(spans, SCORE_KEYS)], finish

    def mix_job(job, state):
        head, _, _, _, spans, _, store = job
        buffer, highest = state["buffer"], state["row"]
        sums = {"totals": None, "mixed": None}

        def piece(begin, at, count):
            span = pl.ds(begin, count)
            rounded = []
            for sub in range(0, count, MIX_STEP):
                part = scores[buffer, pl.ds(at + sub, MIX_STEP), :]
                weights = jnp.exp2((part - highest) * exponent_scale)
                total = jnp.sum(weights.reshape(MIX_STEP // 8, 8, WIDTH), axis=0)
                sums["totals"] = total if sums["totals"] is None else sums["totals"] + total
                rounded.append(weights.astype(jnp.bfloat16))
            mixed = jnp.dot(
                turned[head, :, span], jnp.concatenate(rounded, axis=0), preferred_element_type=jnp.float32
            )
            sums["mixed"] = mixed if sums["mixed"] is None else sums["mixed"] + mixed

        def finish():
            totals = jnp.sum(sums["totals"], axis=0, keepdims=True)
            store(highest * exponent_scale, totals, sums["mixed"])

        return [functools.partial(piece, *cut) for cut in pieces(spans, MIX_KEYS)], finish

    def run(jobs):
        before = None
        for index, job in enumerate(jobs + [None]):
            state, score, score_end, mix, mix_end = None, [], None, [], None
            if job is not None:
                state, score, score_end = score_job(job, index % scores.shape[0])
            if before is not None:
                mix, mix_end = mix_job(*before)
            for step in range(max(len(score), len(mix))):
                if step < len(score):
                    score[step]()
                if step < len(mix):
                    mix[step]()
            if mix_end is not None:
                mix_end()
            if score_end is not None:
                score_end()
            before = (job, state)

    def attend_back(head, step, older, newer):
        jobs = []
        for tile in range(tiles):
            span = pl.ds(tile * TILE, TILE)

            def store(level, totals, mixed, tile=tile, span=span):
                mixed = (mixed * (1.0 / totals)).astype(jnp.bfloat16)
                level = level + jnp.log(totals) * LOG2E
                sent = pl.ds(newer + tile * TILE, TILE)
                for g in range(GROUPS):
                    part = pl.ds(g * DH, DH)
                    turned_back = mixed[:, g * DH : (g + 1) * DH].T
                    slot[step, g, span, :] = jnp.where(next_keys, held[head, g, sent, :], turned_back)
                    stat_out[step, pl.ds(tile * GROUPS + g, 1), :] = jnp.where(
                        next_keys[:1, :], MASKED, level[:, g * DH : (g + 1) * DH]
                    )

            spans = [(older + tile * TILE, rows - tile * TILE), (newer, rows)]
            marks = query_marks[:, pl.ds(rows + tile * TILE, TILE)]
            jobs.append((head, query_back[step, span, :], marks, 0, spans, False, store))
        run(jobs)

    def put(head, span, mixed):
        for g in range(GROUPS):
            out_held[head, span, pl.ds(g * DH, DH)] = mixed[:, g * DH : (g + 1) * DH].T

    def normal(head):
        def store(tile, level, totals, mixed):
            put(head, pl.ds(tile * TILE, TILE), (mixed * (1.0 / totals)).astype(jnp.bfloat16))

        return store

    def keep(side):
        def store(tile, level, totals, mixed):
            kept_mix[side, tile] = mixed
            kept_stat[side, pl.ds(2 * tile, 1), :] = level
            kept_stat[side, pl.ds(2 * tile + 1, 1), :] = totals

        return store

    def merged(head, side, partials):
        def store(tile, level, totals, mixed):
            span = pl.ds(tile * TILE, TILE)
            top = level
            if side is not None:
                local = kept_stat[side, pl.ds(2 * tile, 1), :]
                top = jnp.maximum(top, local)
            if partials:
                other = jnp.concatenate(
                    [stat_in[head, pl.ds(tile * GROUPS + g, 1), :] for g in range(GROUPS)], axis=1
                )
                top = jnp.maximum(top, other)
            here = jnp.exp2(level - top)
            share = totals * here
            if side is not None:
                home = jnp.exp2(local - top)
                share = share + kept_stat[side, pl.ds(2 * tile + 1, 1), :] * home
            if partials:
                there = jnp.exp2(other - top)
                share = share + there
            share = 1.0 / share
            both = mixed * (here * share)
            if side is not None:
                both = both + kept_mix[side, tile] * (home * share)
            if partials:
                sent = pl.ds(rows + tile * TILE, TILE)
                partial = jnp.concatenate([held[head, 0, sent, :].T, turned[head, :, sent]], axis=1)
                both = both + partial.astype(jnp.float32) * (there * share)
            put(head, span, both.astype(jnp.bfloat16))

        return store

    def jobs_of(head, kind, begin_of, end_of, own_end, store):
        jobs = []
        for tile in range(tiles):
            span = pl.ds(tile * TILE, TILE)
            spans = [(begin_of(tile), end_of(tile) - begin_of(tile))]
            end = functools.partial(store, tile)
            jobs.append((head, query_held[head, span, :], query_marks[:, span], kind, spans, own_end, end))
        return jobs

    def at_tile(tile):
        return tile * TILE

    def at_near(tile):
        return rows

    def at_own(tile):
        return 2 * rows

    def past_own(tile):
        return 2 * rows + (tile + 1) * TILE

    last = SPLIT - 1

    @pl.loop(0, HK)
    def _(head):
        turn_values(head, 2 * rows)

    @pl.when(even)
    def _():
        jobs = []
        for side in range(2):
            jobs += jobs_of(side * SPLIT + last, 0, at_own, past_own, True, keep(side))
        run(jobs)

        @pl.loop(1, SPLIT)
        def _(step):
            to_core(step, far).wait_recv()
            turn_values(step, 0)

    @pl.when(odd)
    def _():
        @pl.loop(0, HK)
        def _(head):
            to_core(head, near).wait_recv()
            turn_values(head, rows)

        jobs = []
        for side in range(2):
            jobs += jobs_of(side * SPLIT + last, 0, at_near, past_own, True, keep(side))
        run(jobs)

    @pl.loop(1, SPLIT + 2)
    def _(turn):
        @pl.when(has_next & (turn < SPLIT))
        def _():
            query_to_prev(turn, 0).wait_recv()

            @pl.when(even)
            def _():
                attend_back(turn, turn, 2 * rows, 0)
                slot_to_next(turn, near).start()

            @pl.when(odd)
            def _():
                attend_back(SPLIT + turn, turn, rows, 2 * rows)
                slot_to_next(turn, far).start()

            stat_to_next(turn, core * SPLIT + turn).start()

        @pl.when(turn >= 2)
        def _():
            step = turn - 2

            @pl.when(has_prev)
            def _():
                slot_to_next(step, far).wait_recv()

                @pl.when(even)
                def _():
                    relay(step, near, far).start()

                @pl.when(odd)
                def _():
                    relay(step, far, near).start()

            @pl.loop(0, 2)
            def _(turn_side):
                side = lax.rem(core + turn_side, 2)
                head = side * SPLIT + step

                @pl.when(jnp.logical_and(has_prev, turn_side == 1))
                def _():
                    relay(step, near, far).wait_recv()

                @pl.when(even)
                def _():
                    turn_values(head, rows)

                    @pl.when(step == 0)
                    def _():
                        @pl.when(jnp.logical_and(has_prev, turn_side == 0))
                        def _():
                            first_older(0).wait_recv()

                        @pl.when(jnp.logical_and(has_prev, turn_side == 1))
                        def _():
                            first_older(1).wait_recv()

                        turn_values(head, 0)
                        run(jobs_of(head, 1, at_tile, past_own, True, normal(head)))

                    @pl.when(jnp.logical_and(has_prev, step >= 1))
                    def _():
                        stat_to_next(step, head).wait_recv()

                    @pl.when(jnp.logical_and(step >= 1, step < last))
                    def _():
                        run(jobs_of(head, 0, at_near, past_own, True, merged(head, None, True)))

                    @pl.when(step == last)
                    def _():
                        run(jobs_of(head, 0, at_near, at_own, False, merged(head, side, True)))

                @pl.when(odd)
                def _():
                    turn_values(head, 0)

                    @pl.when(step < last)
                    def _():
                        kind = jnp.where(step == 0, 1, 0)
                        run(jobs_of(head, kind, at_tile, past_own, True, normal(head)))

                    @pl.when(step == last)
                    def _():
                        run(jobs_of(head, 0, at_tile, at_near, False, merged(head, side, False)))

                out_store(head).start()

    @pl.loop(0, HK)
    def _(head):
        out_store(head).wait()

        @pl.when(even)
        def _():
            to_core(head, near).wait_send()

    @pl.when(has_next)
    def _():
        for side in range(2):
            first_older(side).wait_send()

    @pl.loop(0, SPLIT)
    def _(step):
        @pl.when(has_prev)
        def _():
            relay(step, near, far).wait_send()

        @pl.when(step >= 1)
        def _():
            @pl.when(odd)
            def _():
                to_core(step, far).wait_send()

            @pl.when(has_next)
            def _():
                slot_to_next(step, near).wait_send()
                stat_to_next(step, step).wait_send()

            @pl.when(jnp.logical_and(even, has_prev))
            def _():
                for side in range(2):
                    query_to_prev(step, side).wait_send()


def on_device(queries, keys, values, doc_lengths):
    rows = keys.shape[0]
    shards = lax.axis_size("cp")
    window = REACH * rows + TILE
    stats = rows // TILE * GROUPS
    dma = pltpu.SemaphoreType.DMA
    return pl.pallas_call(
        functools.partial(kernel, shards),
        out_shape=jax.ShapeDtypeStruct(queries.shape, queries.dtype),
        in_specs=[
            pl.BlockSpec(memory_space=pltpu.SMEM),
            pl.BlockSpec(memory_space=pl.ANY),
            pl.BlockSpec(memory_space=pl.ANY),
            pl.BlockSpec(memory_space=pl.ANY),
        ],
        out_specs=pl.BlockSpec(memory_space=pl.ANY),
        scratch_shapes=[
            pltpu.VMEM((HK, 2, (REACH + 1) * rows, DH), keys.dtype),
            pltpu.VMEM((HK, rows, WIDTH), queries.dtype),
            pltpu.VMEM((HK, rows, WIDTH), queries.dtype),
            pltpu.VMEM((SPLIT, rows, WIDTH), queries.dtype),
            pltpu.VMEM((SPLIT, 2, rows, DH), keys.dtype),
            pltpu.VMEM((SPLIT, stats, TILE), jnp.float32),
            pltpu.VMEM((HK, stats, TILE), jnp.float32),
            pltpu.VMEM((HK, DH, (REACH + 1) * rows), keys.dtype),
            pltpu.VMEM((2, (REACH + 1) * rows, DH), keys.dtype),
            pltpu.VMEM((DH, 2 * rows), keys.dtype),
            pltpu.VMEM((4, window, WIDTH), jnp.float32),
            pltpu.VMEM((2, rows // TILE, DH, WIDTH), jnp.float32),
            pltpu.VMEM((2, 2 * (rows // TILE), WIDTH), jnp.float32),
            dma((HK, 2)),
            dma((HK,)),
            dma((HK,)),
            dma((HK,)),
            dma((HK,)),
            dma((HK,)),
            dma((SPLIT,)),
            dma((SPLIT,)),
            dma((SPLIT,)),
            dma((2,)),
            dma((2,)),
            dma((SPLIT,)),
            dma((SPLIT,)),
            dma((SPLIT,)),
            dma((HK,)),
        ],
        compiler_params=pltpu.CompilerParams(
            collective_id=0, has_side_effects=True, vmem_limit_bytes=58 * 1024 * 1024
        ),
    )(doc_lengths, queries, keys, values)


def solution(mesh):
    return jax.shard_map(
        on_device,
        mesh=mesh,
        in_specs=(P(("grp", "cp"), None), P(("grp", "cp"), None), P(("grp", "cp"), None), P("grp")),
        out_specs=P(("grp", "cp"), None),
        check_vma=False,
    )
```

```python
import functools
import math

import jax
import jax.numpy as jnp
from jax import lax
from jax.experimental import pallas as pl
from jax.experimental.pallas import tpu as pltpu
from jax.sharding import PartitionSpec as P

HQ = 16
HK = 8
DH = 128
REACH = 2
GROUPS = HQ // HK
WIDTH = GROUPS * DH
TILE = 128
MASKED = -1e30

exponent_scale = 144.0 ** (-0.5) * math.log2(math.e)


LOG2E = math.log2(math.e)
SPLIT = HK // 2
MODULUS = 63
APART = 65536.0
SCORE_KEYS = 640
MIX_KEYS = 256
MIX_STEP = 64
MESH = pl.DeviceIdType.MESH


def kernel(
    shards,
    lengths_ref,
    queries_ref,
    keys_ref,
    values_ref,
    out_ref,
    held,
    query_held,
    query_back,
    slot,
    stat_out,
    stat_in,
    turned,
    key_marks,
    query_marks,
    scores,
    kept_mix,
    kept_stat,
    load_sem,
    query_sem,
    core_send,
    core_recv,
    query_send,
    query_recv,
    slot_send,
    slot_recv,
    first_send,
    first_recv,
    relay_send,
    relay_recv,
    stat_send,
    stat_recv,
    ready,
):
    me = lax.axis_index("cp")
    core = lax.rem(me, 2)
    even = core == 0
    odd = core == 1
    partner = me + 1 - 2 * core
    rows = keys_ref.shape[0]
    docs = lengths_ref.shape[0]
    tiles = rows // TILE
    window = REACH * rows + TILE
    own = pl.ds(REACH * rows, rows)
    near = pl.ds(rows, rows)
    far = pl.ds(0, rows)
    has_prev = me >= 2
    has_next = me < shards - 2
    chip_begin = (me - core) * rows
    next_begin = chip_begin + 2 * rows

    def loads(head):
        lanes = pl.ds(pl.multiple_of(head * DH, DH), DH)
        return (
            pltpu.make_async_copy(keys_ref.at[:, lanes], held.at[head, 0, own], load_sem.at[head, 0]),
            pltpu.make_async_copy(values_ref.at[:, lanes], held.at[head, 1, own], load_sem.at[head, 1]),
        )

    def query_load(head):
        lanes = pl.ds(pl.multiple_of(head * WIDTH, WIDTH), WIDTH)
        return pltpu.make_async_copy(queries_ref.at[:, lanes], query_held.at[head], query_sem.at[head])

    def remote(source, target, send, recv, device):
        return pltpu.make_async_remote_copy(
            src_ref=source,
            dst_ref=target,
            send_sem=send,
            recv_sem=recv,
            device_id={"cp": device},
            device_id_type=MESH,
        )

    def to_core(head, region):
        return remote(
            held.at[head, :, own], held.at[head, :, region], core_send.at[head], core_recv.at[head], partner
        )

    def query_to_prev(step, side):
        return remote(
            query_held.at[side * SPLIT + step],
            query_back.at[step],
            query_send.at[side * SPLIT + step],
            query_recv.at[step],
            me - 2 + side,
        )

    def slot_to_next(step, region):
        return remote(
            slot.at[step],
            held.at[core * SPLIT + step, :, region],
            slot_send.at[step],
            slot_recv.at[step],
            me + 2,
        )

    def first_older():
        return remote(held.at[0, :, own], held.at[0, :, far], first_send, first_recv, me + 2)

    def first_newer():
        return remote(held.at[0, :, own], held.at[0, :, near], first_send, slot_recv.at[0], me + 1)

    def relay(step, source, target):
        head = core * SPLIT + step
        return remote(
            held.at[head, :, source], held.at[head, :, target], relay_send.at[step], relay_recv.at[step], partner
        )

    def stat_to_next(step, head):
        return remote(
            stat_out.at[step], stat_in.at[head], stat_send.at[step], stat_recv.at[head], me + 2 - core
        )

    for copy in loads(0):
        copy.start()
    query_load(SPLIT).start()

    @pl.loop(1, SPLIT)
    def _(step):
        query_load(step).start()
        query_load(SPLIT + step).start()

    @pl.loop(1, HK)
    def _(head):
        for copy in loads(head):
            copy.start()

    query_load(0).start()

    barrier = pltpu.get_barrier_semaphore()

    def greet(device):
        pl.semaphore_signal(barrier, inc=1, device_id={"cp": device}, device_id_type=MESH)

    greet(partner)

    @pl.when(has_prev)
    def _():
        greet(me - 2)

        @pl.when(even)
        def _():
            greet(me - 1)

    next_peers = jnp.where(has_next, 1 + core, 0)
    pl.semaphore_wait(barrier, 1 + next_peers)

    @pl.when(has_next)
    def _():
        pl.semaphore_signal(ready, inc=1, device_id={"cp": me + 2 - core}, device_id_type=MESH)

    for copy in loads(0):
        copy.wait()

    @pl.when(jnp.logical_and(even, has_next))
    def _():
        first_older().start()

    @pl.when(jnp.logical_and(odd, has_next))
    def _():
        first_newer().start()

    @pl.when(jnp.logical_and(even, has_prev))
    def _():
        pl.semaphore_wait(ready, 2)

    query_load(SPLIT).wait()

    @pl.when(jnp.logical_and(even, has_prev))
    def _():
        query_to_prev(0, 1).start()

    @pl.loop(1, SPLIT)
    def _(step):
        for side in range(2):
            query_load(side * SPLIT + step).wait()

            @pl.when(jnp.logical_and(even, has_prev))
            def _():
                query_to_prev(step, side).start()

    @pl.when(even)
    def _():
        to_core(0, near).start()

    @pl.loop(1, HK)
    def _(head):
        for copy in loads(head):
            copy.wait()

        @pl.when(even)
        def _():
            to_core(head, near).start()

        @pl.when(jnp.logical_and(odd, head < SPLIT))
        def _():
            to_core(head, far).start()

    query_load(0).wait()

    @pl.when(jnp.logical_not(has_prev))
    def _():
        @pl.when(even)
        def _():
            held[:, :, near, :] = jnp.zeros((HK, 2, rows, DH), held.dtype)
            held[0, :, far, :] = jnp.zeros((2, rows, DH), held.dtype)
            stat_in[...] = jnp.full(stat_in.shape, MASKED, jnp.float32)

        @pl.when(odd)
        def _():
            held[:, :, far, :] = jnp.zeros((HK, 2, rows, DH), held.dtype)

    row = lax.broadcasted_iota(jnp.int32, (6 * tiles, TILE), 0)
    lane = lax.broadcasted_iota(jnp.int32, (6 * tiles, TILE), 1)
    begins_at = jnp.where(
        row < tiles,
        jnp.where(even, me + 1, me - 2) * rows,
        jnp.where(
            row < 3 * tiles,
            (me - 2) * rows,
            jnp.where(row < 4 * tiles, next_begin - 3 * rows, (me - 6) * rows),
        ),
    )
    positions = begins_at + row * TILE + lane
    edge_row = lax.broadcasted_iota(jnp.int32, (8, TILE), 0)
    edges = jnp.where(edge_row == 0, chip_begin, next_begin)

    def next_docs(step, state):
        end, doc, begins = state
        for k in range(8):
            end = end + lengths_ref[step * 8 + k]
            doc = doc + (positions >= end).astype(jnp.int32)
            begins = jnp.where(edges >= end, end, begins)
        return end, doc, begins

    _, doc, begins = lax.fori_loop(
        0,
        docs // 8,
        next_docs,
        (jnp.int32(0), jnp.zeros(positions.shape, jnp.int32), jnp.zeros(edges.shape, jnp.int32)),
    )
    sends_keys = (edges - begins <= rows).astype(jnp.int32)
    next_keys = jnp.broadcast_to(sends_keys[1:2, :], (TILE, DH)) > 0
    prev_keys = jnp.broadcast_to(sends_keys[0:1, :], positions.shape)
    prev_row = jnp.where(even, 1, 0)
    from_prev = (row >= prev_row * tiles) & (row < (prev_row + 1) * tiles)
    none = (positions < 0) | (from_prev & (prev_keys == 0))
    rest = doc
    for k in range(1, docs // MODULUS + 1):
        rest = rest - jnp.where(doc >= k * MODULUS, MODULUS, 0)
    code_low = jnp.where(none, 2 * DH, doc & (DH // 2 - 1))
    code_high = jnp.where(none, 2 * DH, rest + DH // 2)
    feature = lax.broadcasted_iota(jnp.int32, (DH, TILE), 0)

    def matches(block):
        return (feature == code_low[block : block + 1, :]) | (feature == code_high[block : block + 1, :])

    def mark(block):
        return jnp.where(matches(block), 0.0, -APART).astype(jnp.bfloat16).T

    for block in range(2 * tiles):
        key_marks[0, pl.ds(block * TILE, TILE), :] = mark(block)
        key_marks[1, pl.ds(block * TILE, TILE), :] = mark(4 * tiles + block)
    for block in range(2 * tiles, 3 * tiles):
        for kind in range(2):
            key_marks[kind, pl.ds(block * TILE, TILE), :] = mark(block)
    for block in range(2 * tiles):
        present = jnp.where(matches(2 * tiles + block), 1.0, 0.0).astype(jnp.bfloat16)
        query_marks[:, pl.ds(block * TILE, TILE)] = present

    causal = lax.broadcasted_iota(jnp.int32, (TILE, WIDTH), 0) <= lax.rem(
        lax.broadcasted_iota(jnp.int32, (TILE, WIDTH), 1), TILE
    )

    def turn_values(head, region):
        for tile in range(tiles):
            span = pl.ds(region + tile * TILE, TILE)
            turned[head, :, span] = held[head, 1, span, :].T

    def pieces(spans, size):
        cut, at = [], 0
        for begin, count in spans:
            done = 0
            while done < count:
                step = min(size, count - done)
                cut.append((begin + done, at, step))
                done, at = done + step, at + step
        return cut

    def score_job(job, buffer):
        head, queries, marks, kind, spans, own_end, _ = job
        state = {"highest": None, "buffer": buffer}
        turned_queries = jnp.concatenate([queries[:, g * DH : (g + 1) * DH].T for g in range(GROUPS)], axis=1)
        right = jnp.concatenate([turned_queries, jnp.concatenate([marks] * GROUPS, axis=1)], axis=0)
        total = sum(count for _, count in spans)

        def piece(begin, at, count):
            span = pl.ds(begin, count)
            left = jnp.concatenate([held[head, 0, span, :], key_marks[kind, span, :]], axis=1)
            part = jnp.dot(left, right, preferred_element_type=jnp.float32)
            if own_end and at + count == total:
                last = jnp.where(causal, part[count - TILE :], -APART)
                part = jnp.concatenate([part[: count - TILE], last], axis=0) if count > TILE else last
            scores[buffer, pl.ds(at, count), :] = part
            top = jnp.max(part.reshape(count // 8, 8, WIDTH), axis=0)
            state["highest"] = top if state["highest"] is None else jnp.maximum(state["highest"], top)

        def finish():
            state["row"] = jnp.max(state["highest"], axis=0, keepdims=True)

        return state, [functools.partial(piece, *cut) for cut in pieces(spans, SCORE_KEYS)], finish

    def mix_job(job, state):
        head, _, _, _, spans, _, store = job
        buffer, highest = state["buffer"], state["row"]
        sums = {"totals": None, "mixed": None}

        def piece(begin, at, count):
            span = pl.ds(begin, count)
            rounded = []
            for sub in range(0, count, MIX_STEP):
                part = scores[buffer, pl.ds(at + sub, MIX_STEP), :]
                weights = jnp.exp2((part - highest) * exponent_scale)
                total = jnp.sum(weights.reshape(MIX_STEP // 8, 8, WIDTH), axis=0)
                sums["totals"] = total if sums["totals"] is None else sums["totals"] + total
                rounded.append(weights.astype(jnp.bfloat16))
            mixed = jnp.dot(
                turned[head, :, span], jnp.concatenate(rounded, axis=0), preferred_element_type=jnp.float32
            )
            sums["mixed"] = mixed if sums["mixed"] is None else sums["mixed"] + mixed

        def finish():
            totals = jnp.sum(sums["totals"], axis=0, keepdims=True)
            store(highest * exponent_scale, totals, sums["mixed"])

        return [functools.partial(piece, *cut) for cut in pieces(spans, MIX_KEYS)], finish

    def run(jobs):
        before = None
        for index, job in enumerate(jobs + [None]):
            state, score, score_end, mix, mix_end = None, [], None, [], None
            if job is not None:
                state, score, score_end = score_job(job, index % scores.shape[0])
            if before is not None:
                mix, mix_end = mix_job(*before)
            for step in range(max(len(score), len(mix))):
                if step < len(score):
                    score[step]()
                if step < len(mix):
                    mix[step]()
            if mix_end is not None:
                mix_end()
            if score_end is not None:
                score_end()
            before = (job, state)

    def attend_back(head, step, older, newer):
        jobs = []
        for tile in range(tiles):
            span = pl.ds(tile * TILE, TILE)

            def store(level, totals, mixed, tile=tile, span=span):
                mixed = (mixed * (1.0 / totals)).astype(jnp.bfloat16)
                level = level + jnp.log(totals) * LOG2E
                sent = pl.ds(newer + tile * TILE, TILE)
                for g in range(GROUPS):
                    part = pl.ds(g * DH, DH)
                    turned_back = mixed[:, g * DH : (g + 1) * DH].T
                    slot[step, g, span, :] = jnp.where(next_keys, held[head, g, sent, :], turned_back)
                    stat_out[step, pl.ds(tile * GROUPS + g, 1), :] = jnp.where(
                        next_keys[:1, :], MASKED, level[:, g * DH : (g + 1) * DH]
                    )

            spans = [(older + tile * TILE, rows - tile * TILE), (newer, rows)]
            marks = query_marks[:, pl.ds(rows + tile * TILE, TILE)]
            jobs.append((head, query_back[step, span, :], marks, 0, spans, False, store))
        run(jobs)

    def put(head, span, mixed):
        for g in range(GROUPS):
            lanes = pl.ds(pl.multiple_of(head * WIDTH + g * DH, DH), DH)
            out_ref[span, lanes] = mixed[:, g * DH : (g + 1) * DH].T

    def normal(head):
        def store(tile, level, totals, mixed):
            put(head, pl.ds(tile * TILE, TILE), (mixed * (1.0 / totals)).astype(jnp.bfloat16))

        return store

    def keep(side):
        def store(tile, level, totals, mixed):
            kept_mix[side, tile] = mixed
            kept_stat[side, pl.ds(2 * tile, 1), :] = level
            kept_stat[side, pl.ds(2 * tile + 1, 1), :] = totals

        return store

    def merged(head, side, partials):
        def store(tile, level, totals, mixed):
            span = pl.ds(tile * TILE, TILE)
            top = level
            if side is not None:
                local = kept_stat[side, pl.ds(2 * tile, 1), :]
                top = jnp.maximum(top, local)
            if partials:
                other = jnp.concatenate(
                    [stat_in[head, pl.ds(tile * GROUPS + g, 1), :] for g in range(GROUPS)], axis=1
                )
                top = jnp.maximum(top, other)
            here = jnp.exp2(level - top)
            share = totals * here
            if side is not None:
                home = jnp.exp2(local - top)
                share = share + kept_stat[side, pl.ds(2 * tile + 1, 1), :] * home
            if partials:
                there = jnp.exp2(other - top)
                share = share + there
            share = 1.0 / share
            both = mixed * (here * share)
            if side is not None:
                both = both + kept_mix[side, tile] * (home * share)
            if partials:
                sent = pl.ds(rows + tile * TILE, TILE)
                partial = jnp.concatenate([held[head, 0, sent, :].T, turned[head, :, sent]], axis=1)
                both = both + partial.astype(jnp.float32) * (there * share)
            put(head, span, both.astype(jnp.bfloat16))

        return store

    def jobs_of(head, kind, begin_of, end_of, own_end, store):
        jobs = []
        for tile in range(tiles):
            span = pl.ds(tile * TILE, TILE)
            spans = [(begin_of(tile), end_of(tile) - begin_of(tile))]
            end = functools.partial(store, tile)
            jobs.append((head, query_held[head, span, :], query_marks[:, span], kind, spans, own_end, end))
        return jobs

    def at_tile(tile):
        return tile * TILE

    def at_near(tile):
        return rows

    def at_own(tile):
        return 2 * rows

    def past_own(tile):
        return 2 * rows + (tile + 1) * TILE

    last = SPLIT - 1

    @pl.loop(0, HK)
    def _(head):
        turn_values(head, 2 * rows)

    @pl.when(even)
    def _():
        jobs = []
        for side in range(2):
            jobs += jobs_of(side * SPLIT + last, 0, at_own, past_own, True, keep(side))
        run(jobs)

        @pl.loop(1, SPLIT)
        def _(step):
            to_core(step, far).wait_recv()
            turn_values(step, 0)

    @pl.when(odd)
    def _():
        @pl.loop(0, HK)
        def _(head):
            to_core(head, near).wait_recv()
            turn_values(head, rows)

        jobs = []
        for side in range(2):
            jobs += jobs_of(side * SPLIT + last, 0, at_near, past_own, True, keep(side))
        run(jobs)

    @pl.loop(0, SPLIT + 2)
    def _(turn):
        @pl.when(has_next & even & (turn >= 1) & (turn < SPLIT))
        def _():
            query_to_prev(turn, 0).wait_recv()
            attend_back(turn, turn, 2 * rows, 0)
            slot_to_next(turn, near).start()
            stat_to_next(turn, turn).start()

        @pl.when(has_next & odd & (turn < SPLIT))
        def _():
            query_to_prev(turn, 1).wait_recv()
            attend_back(SPLIT + turn, turn, rows, 2 * rows)
            slot_to_next(turn, far).start()
            stat_to_next(turn, SPLIT + turn).start()

        @pl.when(turn >= 2)
        def _():
            step = turn - 2

            @pl.when(has_prev)
            def _():
                slot_to_next(step, far).wait_recv()

                @pl.when(even)
                def _():
                    relay(step, near, far).start()

                @pl.when(odd)
                def _():
                    relay(step, far, near).start()

            @pl.loop(0, 2)
            def _(turn_side):
                side = lax.rem(core + turn_side, 2)
                head = side * SPLIT + step

                @pl.when(jnp.logical_and(has_prev, turn_side == 1))
                def _():
                    relay(step, near, far).wait_recv()

                @pl.when(even)
                def _():
                    turn_values(head, rows)

                    @pl.when(head == 0)
                    def _():
                        @pl.when(has_prev)
                        def _():
                            first_older().wait_recv()

                        turn_values(0, 0)
                        run(jobs_of(0, 1, at_tile, past_own, True, normal(0)))

                    @pl.when(jnp.logical_and(has_prev, head >= 1))
                    def _():
                        stat_to_next(step, head).wait_recv()

                    @pl.when(jnp.logical_and(head >= 1, step < last))
                    def _():
                        run(jobs_of(head, 0, at_near, past_own, True, merged(head, None, True)))

                    @pl.when(step == last)
                    def _():
                        run(jobs_of(head, 0, at_near, at_own, False, merged(head, side, True)))

                @pl.when(odd)
                def _():
                    turn_values(head, 0)

                    @pl.when(step < last)
                    def _():
                        kind = jnp.where(head == 0, 1, 0)
                        run(jobs_of(head, kind, at_tile, past_own, True, normal(head)))

                    @pl.when(step == last)
                    def _():
                        run(jobs_of(head, 0, at_tile, at_near, False, merged(head, side, False)))

    @pl.when(even)
    def _():
        @pl.loop(0, HK)
        def _(head):
            to_core(head, near).wait_send()

    @pl.when(odd)
    def _():
        @pl.loop(1, SPLIT)
        def _(head):
            to_core(head, far).wait_send()

    @pl.when(has_next)
    def _():
        first_older().wait_send()

        @pl.when(odd)
        def _():
            slot_to_next(0, far).wait_send()
            stat_to_next(0, SPLIT).wait_send()

        @pl.loop(1, SPLIT)
        def _(step):
            slot_to_next(step, near).wait_send()
            stat_to_next(step, step).wait_send()

    @pl.when(has_prev)
    def _():
        @pl.loop(0, SPLIT)
        def _(step):
            relay(step, near, far).wait_send()

        @pl.when(even)
        def _():
            query_to_prev(0, 1).wait_send()

            @pl.loop(1, SPLIT)
            def _(step):
                for side in range(2):
                    query_to_prev(step, side).wait_send()


def on_device(queries, keys, values, doc_lengths):
    rows = keys.shape[0]
    shards = lax.axis_size("cp")
    window = REACH * rows + TILE
    stats = rows // TILE * GROUPS
    dma = pltpu.SemaphoreType.DMA
    return pl.pallas_call(
        functools.partial(kernel, shards),
        out_shape=pltpu.VMEM(queries.shape, queries.dtype),
        in_specs=[
            pl.BlockSpec(memory_space=pltpu.SMEM),
            pl.BlockSpec(memory_space=pl.ANY),
            pl.BlockSpec(memory_space=pl.ANY),
            pl.BlockSpec(memory_space=pl.ANY),
        ],
        out_specs=pl.BlockSpec(memory_space=pltpu.VMEM),
        scratch_shapes=[
            pltpu.VMEM((HK, 2, (REACH + 1) * rows, DH), keys.dtype),
            pltpu.VMEM((HK, rows, WIDTH), queries.dtype),
            pltpu.VMEM((SPLIT, rows, WIDTH), queries.dtype),
            pltpu.VMEM((SPLIT, 2, rows, DH), keys.dtype),
            pltpu.VMEM((SPLIT, stats, TILE), jnp.float32),
            pltpu.VMEM((HK, stats, TILE), jnp.float32),
            pltpu.VMEM((HK, DH, (REACH + 1) * rows), keys.dtype),
            pltpu.VMEM((2, (REACH + 1) * rows, DH), keys.dtype),
            pltpu.VMEM((DH, 2 * rows), keys.dtype),
            pltpu.VMEM((4, window, WIDTH), jnp.float32),
            pltpu.VMEM((2, rows // TILE, DH, WIDTH), jnp.float32),
            pltpu.VMEM((2, 2 * (rows // TILE), WIDTH), jnp.float32),
            dma((HK, 2)),
            dma((HK,)),
            dma((HK,)),
            dma((HK,)),
            dma((HK,)),
            dma((SPLIT,)),
            dma((SPLIT,)),
            dma((SPLIT,)),
            dma(()),
            dma(()),
            dma((SPLIT,)),
            dma((SPLIT,)),
            dma((SPLIT,)),
            dma((HK,)),
            pltpu.SemaphoreType.REGULAR,
        ],
        compiler_params=pltpu.CompilerParams(
            collective_id=0, has_side_effects=True, vmem_limit_bytes=36 * 1024 * 1024
        ),
    )(*(pltpu.with_memory_space_constraint(x, pltpu.HBM) for x in (doc_lengths, queries, keys, values)))


def solution(mesh):
    return jax.shard_map(
        on_device,
        mesh=mesh,
        in_specs=(P(("grp", "cp"), None), P(("grp", "cp"), None), P(("grp", "cp"), None), P("grp")),
        out_specs=P(("grp", "cp"), None),
        check_vma=False,
    )
```

```python
import functools
import math

import jax
import jax.numpy as jnp
from jax import lax
from jax.experimental import pallas as pl
from jax.experimental.pallas import tpu as pltpu
from jax.sharding import PartitionSpec as P

HQ = 16
HK = 8
DH = 128
REACH = 2
GROUPS = HQ // HK
WIDTH = GROUPS * DH
TILE = 128
MASKED = -1e30

exponent_scale = 144.0 ** (-0.5) * math.log2(math.e)


LOG2E = math.log2(math.e)
SPLIT = HK // 2
MODULUS = 63
PARTS = 2
APART = 65536.0
SCORE_KEYS = 640
MIX_KEYS = 256
MIX_STEP = 64
MESH = pl.DeviceIdType.MESH


def kernel(
    shards,
    lengths_ref,
    queries_ref,
    keys_ref,
    values_ref,
    out_ref,
    held,
    query_held,
    query_back,
    slot,
    stat_out,
    stat_in,
    turned,
    key_marks,
    query_marks,
    scores,
    kept_mix,
    kept_stat,
    load_sem,
    query_sem,
    core_send,
    core_recv,
    query_send,
    query_recv,
    slot_send,
    slot_recv,
    first_send,
    first_recv,
    relay_send,
    relay_recv,
    stat_send,
    stat_recv,
    ready,
):
    me = lax.axis_index("cp")
    core = lax.rem(me, 2)
    even = core == 0
    odd = core == 1
    partner = me + 1 - 2 * core
    rows = keys_ref.shape[0]
    docs = lengths_ref.shape[0]
    tiles = rows // TILE
    window = REACH * rows + TILE
    piece_rows = rows // PARTS
    own = pl.ds(REACH * rows, rows)
    near = pl.ds(rows, rows)
    far = pl.ds(0, rows)
    has_prev = me >= 2
    has_next = me < shards - 2
    chip_begin = (me - core) * rows
    next_begin = chip_begin + 2 * rows

    def loads(head):
        lanes = pl.ds(pl.multiple_of(head * DH, DH), DH)
        return (
            pltpu.make_async_copy(keys_ref.at[:, lanes], held.at[head, 0, own], load_sem.at[head, 0]),
            pltpu.make_async_copy(values_ref.at[:, lanes], held.at[head, 1, own], load_sem.at[head, 1]),
        )

    def query_load(head):
        lanes = pl.ds(pl.multiple_of(head * WIDTH, WIDTH), WIDTH)
        return pltpu.make_async_copy(queries_ref.at[:, lanes], query_held.at[head], query_sem.at[head])

    def remote(source, target, send, recv, device):
        return pltpu.make_async_remote_copy(
            src_ref=source,
            dst_ref=target,
            send_sem=send,
            recv_sem=recv,
            device_id={"cp": device},
            device_id_type=MESH,
        )

    def to_core(head, region):
        return remote(
            held.at[head, :, own], held.at[head, :, region], core_send.at[head], core_recv.at[head], partner
        )

    def part_of(region, part):
        return pl.ds(region + part * piece_rows, piece_rows)

    def query_to_prev(step, side, part):
        head = side * SPLIT + step
        return remote(
            query_held.at[head, part_of(0, part)],
            query_back.at[step, part_of(0, part)],
            query_send.at[head, part],
            query_recv.at[step, part],
            me - 2 + side,
        )

    def slot_to_next(step, region, part):
        return remote(
            slot.at[step, :, part_of(0, part)],
            held.at[core * SPLIT + step, :, part_of(region, part)],
            slot_send.at[step, part],
            slot_recv.at[step, part],
            me + 2,
        )

    def first_older(side):
        head = side * SPLIT
        return remote(
            held.at[head, :, own], held.at[head, :, far], first_send.at[side], first_recv.at[side], me + 2
        )

    def first_newer(side):
        head = side * SPLIT
        region = far if side else near
        return remote(
            held.at[head, :, own],
            held.at[head, :, region],
            first_send.at[side],
            first_recv.at[2 + side],
            me + 1 + side,
        )

    def relay(step, source, target, part):
        head = core * SPLIT + step
        return remote(
            held.at[head, :, part_of(source, part)],
            held.at[head, :, part_of(target, part)],
            relay_send.at[step, part],
            relay_recv.at[step, part],
            partner,
        )

    def stat_to_next(step, head):
        return remote(
            stat_out.at[step], stat_in.at[head], stat_send.at[step], stat_recv.at[head], me + 2 - core
        )

    for side in range(2):
        for copy in loads(side * SPLIT):
            copy.start()

    @pl.loop(1, SPLIT)
    def _(step):
        query_load(step).start()
        query_load(SPLIT + step).start()

    @pl.loop(1, SPLIT)
    def _(step):
        for side in range(2):
            for copy in loads(side * SPLIT + step):
                copy.start()

    query_load(0).start()
    query_load(SPLIT).start()

    barrier = pltpu.get_barrier_semaphore()

    def greet(device):
        pl.semaphore_signal(barrier, inc=1, device_id={"cp": device}, device_id_type=MESH)

    greet(partner)

    @pl.when(has_prev)
    def _():
        greet(me - 2)

        @pl.when(even)
        def _():
            greet(me - 1)

    next_peers = jnp.where(has_next, 1 + core, 0)
    pl.semaphore_wait(barrier, 1 + next_peers)

    @pl.when(has_next)
    def _():
        pl.semaphore_signal(ready, inc=1, device_id={"cp": me + 2 - core}, device_id_type=MESH)

    for side in range(2):
        for copy in loads(side * SPLIT):
            copy.wait()

        @pl.when(jnp.logical_and(even, has_next))
        def _():
            first_older(side).start()

        @pl.when(jnp.logical_and(odd, has_next))
        def _():
            first_newer(side).start()

    @pl.when(even)
    def _():
        to_core(0, near).start()
        to_core(SPLIT, near).start()

    @pl.loop(1, SPLIT)
    def _(step):
        for side in range(2):
            head = side * SPLIT + step
            for copy in loads(head):
                copy.wait()

            @pl.when(even)
            def _():
                to_core(head, near).start()

            if side == 0:

                @pl.when(odd)
                def _():
                    to_core(head, far).start()

    @pl.when(jnp.logical_and(even, has_prev))
    def _():
        pl.semaphore_wait(ready, 2)

    @pl.loop(1, SPLIT)
    def _(step):
        for side in range(2):
            query_load(side * SPLIT + step).wait()

            @pl.when(jnp.logical_and(even, has_prev))
            def _():
                for part in range(PARTS):
                    query_to_prev(step, side, part).start()

    query_load(0).wait()
    query_load(SPLIT).wait()

    @pl.when(jnp.logical_not(has_prev))
    def _():
        @pl.when(even)
        def _():
            held[:, :, near, :] = jnp.zeros((HK, 2, rows, DH), held.dtype)
            for side in range(2):
                held[side * SPLIT, :, far, :] = jnp.zeros((2, rows, DH), held.dtype)
            stat_in[...] = jnp.full(stat_in.shape, MASKED, jnp.float32)

        @pl.when(odd)
        def _():
            held[:, :, far, :] = jnp.zeros((HK, 2, rows, DH), held.dtype)

    row = lax.broadcasted_iota(jnp.int32, (6 * tiles, TILE), 0)
    lane = lax.broadcasted_iota(jnp.int32, (6 * tiles, TILE), 1)
    begins_at = jnp.where(
        row < tiles,
        jnp.where(even, me + 1, me - 2) * rows,
        jnp.where(
            row < 3 * tiles,
            (me - 2) * rows,
            jnp.where(row < 4 * tiles, next_begin - 3 * rows, (me - 6) * rows),
        ),
    )
    positions = begins_at + row * TILE + lane
    edge_row = lax.broadcasted_iota(jnp.int32, (8, TILE), 0)
    edges = jnp.where(edge_row == 0, chip_begin, next_begin)

    def next_docs(step, state):
        end, doc, begins = state
        for k in range(8):
            end = end + lengths_ref[step * 8 + k]
            doc = doc + (positions >= end).astype(jnp.int32)
            begins = jnp.where(edges >= end, end, begins)
        return end, doc, begins

    _, doc, begins = lax.fori_loop(
        0,
        docs // 8,
        next_docs,
        (jnp.int32(0), jnp.zeros(positions.shape, jnp.int32), jnp.zeros(edges.shape, jnp.int32)),
    )
    sends_keys = (edges - begins <= rows).astype(jnp.int32)
    next_keys = jnp.broadcast_to(sends_keys[1:2, :], (TILE, DH)) > 0
    prev_keys = jnp.broadcast_to(sends_keys[0:1, :], positions.shape)
    prev_row = jnp.where(even, 1, 0)
    from_prev = (row >= prev_row * tiles) & (row < (prev_row + 1) * tiles)
    none = (positions < 0) | (from_prev & (prev_keys == 0))
    rest = doc
    for k in range(1, docs // MODULUS + 1):
        rest = rest - jnp.where(doc >= k * MODULUS, MODULUS, 0)
    code_low = jnp.where(none, 2 * DH, doc & (DH // 2 - 1))
    code_high = jnp.where(none, 2 * DH, rest + DH // 2)
    feature = lax.broadcasted_iota(jnp.int32, (DH, TILE), 0)

    def matches(block):
        return (feature == code_low[block : block + 1, :]) | (feature == code_high[block : block + 1, :])

    def mark(block):
        return jnp.where(matches(block), 0.0, -APART).astype(jnp.bfloat16).T

    for block in range(2 * tiles):
        key_marks[0, pl.ds(block * TILE, TILE), :] = mark(block)
        key_marks[1, pl.ds(block * TILE, TILE), :] = mark(4 * tiles + block)
    for block in range(2 * tiles, 3 * tiles):
        for kind in range(2):
            key_marks[kind, pl.ds(block * TILE, TILE), :] = mark(block)
    for block in range(2 * tiles):
        present = jnp.where(matches(2 * tiles + block), 1.0, 0.0).astype(jnp.bfloat16)
        query_marks[:, pl.ds(block * TILE, TILE)] = present

    causal = lax.broadcasted_iota(jnp.int32, (TILE, WIDTH), 0) <= lax.rem(
        lax.broadcasted_iota(jnp.int32, (TILE, WIDTH), 1), TILE
    )

    def turn_values(head, region):
        for tile in range(tiles):
            span = pl.ds(region + tile * TILE, TILE)
            turned[head, :, span] = held[head, 1, span, :].T

    def pieces(spans, size):
        cut, at = [], 0
        for begin, count in spans:
            done = 0
            while done < count:
                step = min(size, count - done)
                cut.append((begin + done, at, step))
                done, at = done + step, at + step
        return cut

    def score_job(job, buffer):
        head, queries, marks, kind, spans, own_end, _ = job
        state = {"highest": None, "buffer": buffer}
        turned_queries = jnp.concatenate([queries[:, g * DH : (g + 1) * DH].T for g in range(GROUPS)], axis=1)
        right = jnp.concatenate([turned_queries, jnp.concatenate([marks] * GROUPS, axis=1)], axis=0)
        total = sum(count for _, count in spans)

        def piece(begin, at, count):
            span = pl.ds(begin, count)
            left = jnp.concatenate([held[head, 0, span, :], key_marks[kind, span, :]], axis=1)
            part = jnp.dot(left, right, preferred_element_type=jnp.float32)
            if own_end and at + count == total:
                last = jnp.where(causal, part[count - TILE :], -APART)
                part = jnp.concatenate([part[: count - TILE], last], axis=0) if count > TILE else last
            scores[buffer, pl.ds(at, count), :] = part
            top = jnp.max(part.reshape(count // 8, 8, WIDTH), axis=0)
            state["highest"] = top if state["highest"] is None else jnp.maximum(state["highest"], top)

        def finish():
            state["row"] = jnp.max(state["highest"], axis=0, keepdims=True)

        return state, [functools.partial(piece, *cut) for cut in pieces(spans, SCORE_KEYS if own_end else 256)], finish

    def mix_job(job, state):
        head, _, _, _, spans, _, store = job
        buffer, highest = state["buffer"], state["row"]
        sums = {"totals": None, "mixed": None}

        def piece(begin, at, count):
            span = pl.ds(begin, count)
            rounded = []
            for sub in range(0, count, MIX_STEP):
                part = scores[buffer, pl.ds(at + sub, MIX_STEP), :]
                weights = jnp.exp2((part - highest) * exponent_scale)
                total = jnp.sum(weights.reshape(MIX_STEP // 8, 8, WIDTH), axis=0)
                sums["totals"] = total if sums["totals"] is None else sums["totals"] + total
                rounded.append(weights.astype(jnp.bfloat16))
            mixed = jnp.dot(
                turned[head, :, span], jnp.concatenate(rounded, axis=0), preferred_element_type=jnp.float32
            )
            sums["mixed"] = mixed if sums["mixed"] is None else sums["mixed"] + mixed

        def finish():
            totals = jnp.sum(sums["totals"], axis=0, keepdims=True)
            store(highest * exponent_scale, totals, sums["mixed"])

        return [functools.partial(piece, *cut) for cut in pieces(spans, MIX_KEYS)], finish

    def run(jobs):
        before = None
        for index, job in enumerate(jobs + [None]):
            state, score, score_end, mix, mix_end = None, [], None, [], None
            if job is not None:
                state, score, score_end = score_job(job, index % scores.shape[0])
            if before is not None:
                mix, mix_end = mix_job(*before)
            for step in range(max(len(score), len(mix))):
                if step < len(score):
                    score[step]()
                if step < len(mix):
                    mix[step]()
            if mix_end is not None:
                mix_end()
            if score_end is not None:
                score_end()
            before = (job, state)

    def attend_back(head, step, older, newer, part):
        jobs = []
        for tile in range(part * tiles // PARTS, (part + 1) * tiles // PARTS):
            span = pl.ds(tile * TILE, TILE)

            def store(level, totals, mixed, tile=tile, span=span):
                mixed = (mixed * (1.0 / totals)).astype(jnp.bfloat16)
                level = level + jnp.log(totals) * LOG2E
                sent = pl.ds(newer + tile * TILE, TILE)
                for g in range(GROUPS):
                    part = pl.ds(g * DH, DH)
                    turned_back = mixed[:, g * DH : (g + 1) * DH].T
                    slot[step, g, span, :] = jnp.where(next_keys, held[head, g, sent, :], turned_back)
                    stat_out[step, pl.ds(tile * GROUPS + g, 1), :] = jnp.where(
                        next_keys[:1, :], MASKED, level[:, g * DH : (g + 1) * DH]
                    )

            spans = [(older + tile * TILE, rows - tile * TILE), (newer, rows)]
            marks = query_marks[:, pl.ds(rows + tile * TILE, TILE)]
            jobs.append((head, query_back[step, span, :], marks, 0, spans, False, store))
        run(jobs)

    def put(head, span, mixed):
        for g in range(GROUPS):
            lanes = pl.ds(pl.multiple_of(head * WIDTH + g * DH, DH), DH)
            out_ref[span, lanes] = mixed[:, g * DH : (g + 1) * DH].T

    def normal(head):
        def store(tile, level, totals, mixed):
            put(head, pl.ds(tile * TILE, TILE), (mixed * (1.0 / totals)).astype(jnp.bfloat16))

        return store

    def keep(side):
        def store(tile, level, totals, mixed):
            kept_mix[side, tile] = mixed
            kept_stat[side, pl.ds(2 * tile, 1), :] = level
            kept_stat[side, pl.ds(2 * tile + 1, 1), :] = totals

        return store

    def merged(head, side, partials):
        def store(tile, level, totals, mixed):
            span = pl.ds(tile * TILE, TILE)
            top = level
            if side is not None:
                local = kept_stat[side, pl.ds(2 * tile, 1), :]
                top = jnp.maximum(top, local)
            if partials:
                other = jnp.concatenate(
                    [stat_in[head, pl.ds(tile * GROUPS + g, 1), :] for g in range(GROUPS)], axis=1
                )
                top = jnp.maximum(top, other)
            here = jnp.exp2(level - top)
            share = totals * here
            if side is not None:
                home = jnp.exp2(local - top)
                share = share + kept_stat[side, pl.ds(2 * tile + 1, 1), :] * home
            if partials:
                there = jnp.exp2(other - top)
                share = share + there
            share = 1.0 / share
            both = mixed * (here * share)
            if side is not None:
                both = both + kept_mix[side, tile] * (home * share)
            if partials:
                sent = pl.ds(rows + tile * TILE, TILE)
                partial = jnp.concatenate([held[head, 0, sent, :].T, turned[head, :, sent]], axis=1)
                both = both + partial.astype(jnp.float32) * (there * share)
            put(head, span, both.astype(jnp.bfloat16))

        return store

    def jobs_of(head, kind, begin_of, end_of, own_end, store):
        jobs = []
        for tile in range(tiles):
            span = pl.ds(tile * TILE, TILE)
            spans = [(begin_of(tile), end_of(tile) - begin_of(tile))]
            end = functools.partial(store, tile)
            jobs.append((head, query_held[head, span, :], query_marks[:, span], kind, spans, own_end, end))
        return jobs

    def at_tile(tile):
        return tile * TILE

    def at_near(tile):
        return rows

    def at_own(tile):
        return 2 * rows

    def past_own(tile):
        return 2 * rows + (tile + 1) * TILE

    early = SPLIT - 2

    @pl.loop(0, HK)
    def _(head):
        turn_values(head, 2 * rows)

    @pl.when(even)
    def _():
        @pl.loop(1, SPLIT)
        def _(step):
            to_core(step, far).wait_recv()
            turn_values(step, 0)

    @pl.when(odd)
    def _():
        @pl.loop(0, HK)
        def _(head):
            to_core(head, near).wait_recv()
            turn_values(head, rows)

    @pl.loop(0, SPLIT + 3)
    def _(count):
        turn = count - 1

        @pl.when(has_next & even & (turn >= 1) & (turn < SPLIT))
        def _():
            for part in range(PARTS):
                query_to_prev(turn, 0, part).wait_recv()
                attend_back(turn, turn, 2 * rows, 0, part)
                slot_to_next(turn, rows, part).start()

            stat_to_next(turn, turn).start()

        @pl.when(has_next & odd & (turn >= 1) & (turn < SPLIT))
        def _():
            for part in range(PARTS):
                query_to_prev(turn, 1, part).wait_recv()
                attend_back(SPLIT + turn, turn, rows, 2 * rows, part)
                slot_to_next(turn, 0, part).start()

            stat_to_next(turn, SPLIT + turn).start()

        for which, begin in ((even, at_own), (odd, at_near)):

            @pl.when(which & (turn <= 0))
            def _():
                jobs = []
                for side in range(2):
                    head = side * SPLIT + early - turn
                    jobs += jobs_of(head, 0, begin, past_own, True, keep(-2 * turn + side))
                run(jobs)

        @pl.when(turn >= 2)
        def _():
            step = turn - 2

            @pl.when(has_prev)
            def _():
                @pl.when(jnp.logical_and(even, step == 0))
                def _():
                    first_newer(0).wait_recv()
                    for part in range(PARTS):
                        relay(step, rows, 0, part).start()

                @pl.when(jnp.logical_and(odd, step == 0))
                def _():
                    first_newer(1).wait_recv()
                    for part in range(PARTS):
                        relay(step, 0, rows, part).start()

                @pl.when(jnp.logical_and(even, step >= 1))
                def _():
                    for part in range(PARTS):
                        slot_to_next(step, rows, part).wait_recv()
                        relay(step, rows, 0, part).start()

                @pl.when(jnp.logical_and(odd, step >= 1))
                def _():
                    for part in range(PARTS):
                        slot_to_next(step, 0, part).wait_recv()
                        relay(step, 0, rows, part).start()

            @pl.loop(0, 2)
            def _(turn_side):
                side = lax.rem(core + turn_side, 2)
                head = side * SPLIT + step

                @pl.when(jnp.logical_and(has_prev, turn_side == 1))
                def _():
                    for part in range(PARTS):
                        relay(step, 0, rows, part).wait_recv()

                @pl.when(even)
                def _():
                    turn_values(head, rows)

                    @pl.when(step == 0)
                    def _():
                        @pl.when(jnp.logical_and(has_prev, turn_side == 0))
                        def _():
                            first_older(0).wait_recv()

                        @pl.when(jnp.logical_and(has_prev, turn_side == 1))
                        def _():
                            first_older(1).wait_recv()

                        turn_values(head, 0)
                        run(jobs_of(head, 1, at_tile, past_own, True, normal(head)))

                    @pl.when(jnp.logical_and(has_prev, step >= 1))
                    def _():
                        stat_to_next(step, head).wait_recv()

                    @pl.when(jnp.logical_and(step >= 1, step < early))
                    def _():
                        run(jobs_of(head, 0, at_near, past_own, True, merged(head, None, True)))

                    @pl.when(step >= early)
                    def _():
                        run(jobs_of(head, 0, at_near, at_own, False, merged(head, 2 * (step - early) + side, True)))

                @pl.when(odd)
                def _():
                    turn_values(head, 0)

                    @pl.when(step < early)
                    def _():
                        kind = jnp.where(step == 0, 1, 0)
                        run(jobs_of(head, kind, at_tile, past_own, True, normal(head)))

                    @pl.when(step >= early)
                    def _():
                        run(jobs_of(head, 0, at_tile, at_near, False, merged(head, 2 * (step - early) + side, False)))

    @pl.when(even)
    def _():
        @pl.loop(0, HK)
        def _(head):
            to_core(head, near).wait_send()

    @pl.when(odd)
    def _():
        @pl.loop(1, SPLIT)
        def _(head):
            to_core(head, far).wait_send()

    @pl.when(has_next)
    def _():
        for side in range(2):
            first_older(side).wait_send()

        @pl.loop(1, SPLIT)
        def _(step):
            for part in range(PARTS):
                slot_to_next(step, 0, part).wait_send()
            stat_to_next(step, step).wait_send()

    @pl.when(has_prev)
    def _():
        @pl.loop(0, SPLIT)
        def _(step):
            for part in range(PARTS):
                relay(step, 0, rows, part).wait_send()

        @pl.when(even)
        def _():
            @pl.loop(1, SPLIT)
            def _(step):
                for side in range(2):
                    for part in range(PARTS):
                        query_to_prev(step, side, part).wait_send()


def on_device(queries, keys, values, doc_lengths):
    rows = keys.shape[0]
    shards = lax.axis_size("cp")
    window = REACH * rows + TILE
    stats = rows // TILE * GROUPS
    dma = pltpu.SemaphoreType.DMA
    return pl.pallas_call(
        functools.partial(kernel, shards),
        out_shape=pltpu.VMEM(queries.shape, queries.dtype),
        in_specs=[
            pl.BlockSpec(memory_space=pltpu.SMEM),
            pl.BlockSpec(memory_space=pl.ANY),
            pl.BlockSpec(memory_space=pl.ANY),
            pl.BlockSpec(memory_space=pl.ANY),
        ],
        out_specs=pl.BlockSpec(memory_space=pltpu.VMEM),
        scratch_shapes=[
            pltpu.VMEM((HK, 2, (REACH + 1) * rows, DH), keys.dtype),
            pltpu.VMEM((HK, rows, WIDTH), queries.dtype),
            pltpu.VMEM((SPLIT, rows, WIDTH), queries.dtype),
            pltpu.VMEM((SPLIT, 2, rows, DH), keys.dtype),
            pltpu.VMEM((SPLIT, stats, TILE), jnp.float32),
            pltpu.VMEM((HK, stats, TILE), jnp.float32),
            pltpu.VMEM((HK, DH, (REACH + 1) * rows), keys.dtype),
            pltpu.VMEM((2, (REACH + 1) * rows, DH), keys.dtype),
            pltpu.VMEM((DH, 2 * rows), keys.dtype),
            pltpu.VMEM((4, window, WIDTH), jnp.float32),
            pltpu.VMEM((4, rows // TILE, DH, WIDTH), jnp.float32),
            pltpu.VMEM((4, 2 * (rows // TILE), WIDTH), jnp.float32),
            dma((HK, 2)),
            dma((HK,)),
            dma((HK,)),
            dma((HK,)),
            dma((HK, PARTS)),
            dma((SPLIT, PARTS)),
            dma((SPLIT, PARTS)),
            dma((SPLIT, PARTS)),
            dma((2,)),
            dma((4,)),
            dma((SPLIT, PARTS)),
            dma((SPLIT, PARTS)),
            dma((SPLIT,)),
            dma((HK,)),
            pltpu.SemaphoreType.REGULAR,
        ],
        compiler_params=pltpu.CompilerParams(
            collective_id=0, has_side_effects=True, vmem_limit_bytes=36 * 1024 * 1024
        ),
    )(*(pltpu.with_memory_space_constraint(x, pltpu.HBM) for x in (doc_lengths, queries, keys, values)))


def solution(mesh):
    return jax.shard_map(
        on_device,
        mesh=mesh,
        in_specs=(P(("grp", "cp"), None), P(("grp", "cp"), None), P(("grp", "cp"), None), P("grp")),
        out_specs=P(("grp", "cp"), None),
        check_vma=False,
    )
```

```python
import functools
import math

import jax
import jax.numpy as jnp
from jax import lax
from jax.experimental import pallas as pl
from jax.experimental.pallas import tpu as pltpu
from jax.sharding import PartitionSpec as P

HQ = 16
HK = 8
DH = 128
REACH = 2
GROUPS = HQ // HK
WIDTH = GROUPS * DH
TILE = 128
MASKED = -1e30

exponent_scale = 144.0 ** (-0.5) * math.log2(math.e)


LOG2E = math.log2(math.e)
SPLIT = HK // 2
MODULUS = 63
PARTS = 1
APART = 65536.0
SCORE_KEYS = 640
MIX_KEYS = 256
MIX_STEP = 64
MESH = pl.DeviceIdType.MESH


def kernel(
    shards,
    lengths_ref,
    queries_ref,
    keys_ref,
    values_ref,
    out_ref,
    held,
    query_held,
    query_back,
    slot,
    stat_out,
    stat_in,
    turned,
    key_marks,
    query_marks,
    scores,
    kept_mix,
    kept_stat,
    load_sem,
    query_sem,
    core_send,
    core_recv,
    query_send,
    query_recv,
    slot_send,
    slot_recv,
    first_send,
    first_recv,
    relay_send,
    relay_recv,
    stat_send,
    stat_recv,
    ready,
):
    me = lax.axis_index("cp")
    core = lax.rem(me, 2)
    even = core == 0
    odd = core == 1
    partner = me + 1 - 2 * core
    rows = keys_ref.shape[0]
    docs = lengths_ref.shape[0]
    tiles = rows // TILE
    window = REACH * rows + TILE
    piece_rows = rows // PARTS
    own = pl.ds(REACH * rows, rows)
    near = pl.ds(rows, rows)
    far = pl.ds(0, rows)
    has_prev = me >= 2
    has_next = me < shards - 2
    chip_begin = (me - core) * rows
    next_begin = chip_begin + 2 * rows

    def loads(head):
        lanes = pl.ds(pl.multiple_of(head * DH, DH), DH)
        return (
            pltpu.make_async_copy(keys_ref.at[:, lanes], held.at[head, 0, own], load_sem.at[head, 0]),
            pltpu.make_async_copy(values_ref.at[:, lanes], held.at[head, 1, own], load_sem.at[head, 1]),
        )

    def query_load(head):
        lanes = pl.ds(pl.multiple_of(head * WIDTH, WIDTH), WIDTH)
        return pltpu.make_async_copy(queries_ref.at[:, lanes], query_held.at[head], query_sem.at[head])

    def remote(source, target, send, recv, device):
        return pltpu.make_async_remote_copy(
            src_ref=source,
            dst_ref=target,
            send_sem=send,
            recv_sem=recv,
            device_id={"cp": device},
            device_id_type=MESH,
        )

    def to_core(head, region):
        return remote(
            held.at[head, :, own], held.at[head, :, region], core_send.at[head], core_recv.at[head], partner
        )

    def part_of(region, part):
        return pl.ds(region + part * piece_rows, piece_rows)

    def query_to_prev(step, side, part):
        head = side * SPLIT + step
        return remote(
            query_held.at[head, part_of(0, part)],
            query_back.at[step, part_of(0, part)],
            query_send.at[head, part],
            query_recv.at[step, part],
            me - 2 + side,
        )

    def slot_to_next(step, region, part):
        return remote(
            slot.at[step, :, part_of(0, part)],
            held.at[core * SPLIT + step, :, part_of(region, part)],
            slot_send.at[step, part],
            slot_recv.at[step, part],
            me + 2,
        )

    def first_older(side):
        head = side * SPLIT
        return remote(
            held.at[head, :, own], held.at[head, :, far], first_send.at[side], first_recv.at[side], me + 2
        )

    def first_newer(side):
        head = side * SPLIT
        region = far if side else near
        return remote(
            held.at[head, :, own],
            held.at[head, :, region],
            first_send.at[side],
            first_recv.at[2 + side],
            me + 1 + side,
        )

    def relay(step, source, target, part):
        head = core * SPLIT + step
        return remote(
            held.at[head, :, part_of(source, part)],
            held.at[head, :, part_of(target, part)],
            relay_send.at[step, part],
            relay_recv.at[step, part],
            partner,
        )

    def stat_to_next(step, head):
        return remote(
            stat_out.at[step], stat_in.at[head], stat_send.at[step], stat_recv.at[head], me + 2 - core
        )

    for side in range(2):
        for copy in loads(side * SPLIT):
            copy.start()

    @pl.loop(1, SPLIT)
    def _(step):
        query_load(step).start()
        query_load(SPLIT + step).start()

    @pl.loop(1, SPLIT)
    def _(step):
        for side in range(2):
            for copy in loads(side * SPLIT + step):
                copy.start()

    query_load(0).start()
    query_load(SPLIT).start()

    barrier = pltpu.get_barrier_semaphore()

    def greet(device):
        pl.semaphore_signal(barrier, inc=1, device_id={"cp": device}, device_id_type=MESH)

    greet(partner)

    @pl.when(has_prev)
    def _():
        greet(me - 2)

        @pl.when(even)
        def _():
            greet(me - 1)

    next_peers = jnp.where(has_next, 1 + core, 0)
    pl.semaphore_wait(barrier, 1 + next_peers)

    @pl.when(has_next)
    def _():
        pl.semaphore_signal(ready, inc=1, device_id={"cp": me + 2 - core}, device_id_type=MESH)

    for side in range(2):
        for copy in loads(side * SPLIT):
            copy.wait()

        @pl.when(jnp.logical_and(even, has_next))
        def _():
            first_older(side).start()

        @pl.when(jnp.logical_and(odd, has_next))
        def _():
            first_newer(side).start()

    @pl.when(even)
    def _():
        to_core(0, near).start()
        to_core(SPLIT, near).start()

    @pl.loop(1, SPLIT)
    def _(step):
        for side in range(2):
            head = side * SPLIT + step
            for copy in loads(head):
                copy.wait()

            @pl.when(even)
            def _():
                to_core(head, near).start()

            if side == 0:

                @pl.when(odd)
                def _():
                    to_core(head, far).start()

    @pl.when(jnp.logical_and(even, has_prev))
    def _():
        pl.semaphore_wait(ready, 2)

    @pl.loop(1, SPLIT)
    def _(step):
        for side in range(2):
            query_load(side * SPLIT + step).wait()

            @pl.when(jnp.logical_and(even, has_prev))
            def _():
                for part in range(PARTS):
                    query_to_prev(step, side, part).start()

    query_load(0).wait()
    query_load(SPLIT).wait()

    @pl.when(jnp.logical_not(has_prev))
    def _():
        @pl.when(even)
        def _():
            held[:, :, near, :] = jnp.zeros((HK, 2, rows, DH), held.dtype)
            for side in range(2):
                held[side * SPLIT, :, far, :] = jnp.zeros((2, rows, DH), held.dtype)
            stat_in[...] = jnp.full(stat_in.shape, MASKED, jnp.float32)

        @pl.when(odd)
        def _():
            held[:, :, far, :] = jnp.zeros((HK, 2, rows, DH), held.dtype)

    row = lax.broadcasted_iota(jnp.int32, (6 * tiles, TILE), 0)
    lane = lax.broadcasted_iota(jnp.int32, (6 * tiles, TILE), 1)
    begins_at = jnp.where(
        row < tiles,
        jnp.where(even, me + 1, me - 2) * rows,
        jnp.where(
            row < 3 * tiles,
            (me - 2) * rows,
            jnp.where(row < 4 * tiles, next_begin - 3 * rows, (me - 6) * rows),
        ),
    )
    positions = begins_at + row * TILE + lane
    edge_row = lax.broadcasted_iota(jnp.int32, (8, TILE), 0)
    edges = jnp.where(edge_row == 0, chip_begin, next_begin)

    def next_docs(step, state):
        end, doc, begins = state
        for k in range(8):
            end = end + lengths_ref[step * 8 + k]
            doc = doc + (positions >= end).astype(jnp.int32)
            begins = jnp.where(edges >= end, end, begins)
        return end, doc, begins

    _, doc, begins = lax.fori_loop(
        0,
        docs // 8,
        next_docs,
        (jnp.int32(0), jnp.zeros(positions.shape, jnp.int32), jnp.zeros(edges.shape, jnp.int32)),
    )
    sends_keys = (edges - begins <= rows).astype(jnp.int32)
    next_keys = jnp.broadcast_to(sends_keys[1:2, :], (TILE, DH)) > 0
    prev_keys = jnp.broadcast_to(sends_keys[0:1, :], positions.shape)
    prev_row = jnp.where(even, 1, 0)
    from_prev = (row >= prev_row * tiles) & (row < (prev_row + 1) * tiles)
    none = (positions < 0) | (from_prev & (prev_keys == 0))
    rest = doc
    for k in range(1, docs // MODULUS + 1):
        rest = rest - jnp.where(doc >= k * MODULUS, MODULUS, 0)
    code_low = jnp.where(none, 2 * DH, doc & (DH // 2 - 1))
    code_high = jnp.where(none, 2 * DH, rest + DH // 2)
    feature = lax.broadcasted_iota(jnp.int32, (DH, TILE), 0)

    def matches(block):
        return (feature == code_low[block : block + 1, :]) | (feature == code_high[block : block + 1, :])

    def mark(block):
        return jnp.where(matches(block), 0.0, -APART).astype(jnp.bfloat16).T

    for block in range(2 * tiles):
        key_marks[0, pl.ds(block * TILE, TILE), :] = mark(block)
        key_marks[1, pl.ds(block * TILE, TILE), :] = mark(4 * tiles + block)
    for block in range(2 * tiles, 3 * tiles):
        for kind in range(2):
            key_marks[kind, pl.ds(block * TILE, TILE), :] = mark(block)
    for block in range(2 * tiles):
        present = jnp.where(matches(2 * tiles + block), 1.0, 0.0).astype(jnp.bfloat16)
        query_marks[:, pl.ds(block * TILE, TILE)] = present

    causal = lax.broadcasted_iota(jnp.int32, (TILE, WIDTH), 0) <= lax.rem(
        lax.broadcasted_iota(jnp.int32, (TILE, WIDTH), 1), TILE
    )

    def turn_values(head, region):
        for tile in range(tiles):
            span = pl.ds(region + tile * TILE, TILE)
            turned[head, :, span] = held[head, 1, span, :].T

    def pieces(spans, size):
        cut, at = [], 0
        for begin, count in spans:
            done = 0
            while done < count:
                step = min(size, count - done)
                cut.append((begin + done, at, step))
                done, at = done + step, at + step
        return cut

    def score_job(job, buffer):
        head, queries, marks, kind, spans, own_end, _ = job
        state = {"highest": None, "buffer": buffer}
        turned_queries = jnp.concatenate([queries[:, g * DH : (g + 1) * DH].T for g in range(GROUPS)], axis=1)
        right = jnp.concatenate([turned_queries, jnp.concatenate([marks] * GROUPS, axis=1)], axis=0)
        total = sum(count for _, count in spans)

        def piece(begin, at, count):
            span = pl.ds(begin, count)
            left = jnp.concatenate([held[head, 0, span, :], key_marks[kind, span, :]], axis=1)
            part = jnp.dot(left, right, preferred_element_type=jnp.float32)
            if own_end and at + count == total:
                last = jnp.where(causal, part[count - TILE :], -APART)
                part = jnp.concatenate([part[: count - TILE], last], axis=0) if count > TILE else last
            scores[buffer, pl.ds(at, count), :] = part
            top = jnp.max(part.reshape(count // 8, 8, WIDTH), axis=0)
            state["highest"] = top if state["highest"] is None else jnp.maximum(state["highest"], top)

        def finish():
            state["row"] = jnp.max(state["highest"], axis=0, keepdims=True)

        return state, [functools.partial(piece, *cut) for cut in pieces(spans, SCORE_KEYS if own_end else 256)], finish

    def mix_job(job, state):
        head, _, _, _, spans, _, store = job
        buffer, highest = state["buffer"], state["row"]
        sums = {"totals": None, "mixed": None}

        def piece(begin, at, count):
            span = pl.ds(begin, count)
            rounded = []
            for sub in range(0, count, MIX_STEP):
                part = scores[buffer, pl.ds(at + sub, MIX_STEP), :]
                weights = jnp.exp2((part - highest) * exponent_scale)
                total = jnp.sum(weights.reshape(MIX_STEP // 8, 8, WIDTH), axis=0)
                sums["totals"] = total if sums["totals"] is None else sums["totals"] + total
                rounded.append(weights.astype(jnp.bfloat16))
            mixed = jnp.dot(
                turned[head, :, span], jnp.concatenate(rounded, axis=0), preferred_element_type=jnp.float32
            )
            sums["mixed"] = mixed if sums["mixed"] is None else sums["mixed"] + mixed

        def finish():
            totals = jnp.sum(sums["totals"], axis=0, keepdims=True)
            store(highest * exponent_scale, totals, sums["mixed"])

        return [functools.partial(piece, *cut) for cut in pieces(spans, MIX_KEYS)], finish

    def run(jobs):
        before = None
        for index, job in enumerate(jobs + [None]):
            state, score, score_end, mix, mix_end = None, [], None, [], None
            if job is not None:
                state, score, score_end = score_job(job, index % scores.shape[0])
            if before is not None:
                mix, mix_end = mix_job(*before)
            for step in range(max(len(score), len(mix))):
                if step < len(score):
                    score[step]()
                if step < len(mix):
                    mix[step]()
            if mix_end is not None:
                mix_end()
            if score_end is not None:
                score_end()
            before = (job, state)

    def attend_back(head, step, older, newer, part):
        jobs = []
        for tile in range(part * tiles // PARTS, (part + 1) * tiles // PARTS):
            span = pl.ds(tile * TILE, TILE)

            def store(level, totals, mixed, tile=tile, span=span):
                mixed = (mixed * (1.0 / totals)).astype(jnp.bfloat16)
                level = level + jnp.log(totals) * LOG2E
                sent = pl.ds(newer + tile * TILE, TILE)
                for g in range(GROUPS):
                    part = pl.ds(g * DH, DH)
                    turned_back = mixed[:, g * DH : (g + 1) * DH].T
                    slot[step, g, span, :] = jnp.where(next_keys, held[head, g, sent, :], turned_back)
                    stat_out[step, pl.ds(tile * GROUPS + g, 1), :] = jnp.where(
                        next_keys[:1, :], MASKED, level[:, g * DH : (g + 1) * DH]
                    )

            spans = [(older + tile * TILE, rows - tile * TILE), (newer, rows)]
            marks = query_marks[:, pl.ds(rows + tile * TILE, TILE)]
            jobs.append((head, query_back[step, span, :], marks, 0, spans, False, store))
        run(jobs)

    def put(head, span, mixed):
        for g in range(GROUPS):
            lanes = pl.ds(pl.multiple_of(head * WIDTH + g * DH, DH), DH)
            out_ref[span, lanes] = mixed[:, g * DH : (g + 1) * DH].T

    def normal(head):
        def store(tile, level, totals, mixed):
            put(head, pl.ds(tile * TILE, TILE), (mixed * (1.0 / totals)).astype(jnp.bfloat16))

        return store

    def keep(side):
        def store(tile, level, totals, mixed):
            kept_mix[side, tile] = mixed
            kept_stat[side, pl.ds(2 * tile, 1), :] = level
            kept_stat[side, pl.ds(2 * tile + 1, 1), :] = totals

        return store

    def merged(head, side, partials):
        def store(tile, level, totals, mixed):
            span = pl.ds(tile * TILE, TILE)
            top = level
            if side is not None:
                local = kept_stat[side, pl.ds(2 * tile, 1), :]
                top = jnp.maximum(top, local)
            if partials:
                other = jnp.concatenate(
                    [stat_in[head, pl.ds(tile * GROUPS + g, 1), :] for g in range(GROUPS)], axis=1
                )
                top = jnp.maximum(top, other)
            here = jnp.exp2(level - top)
            share = totals * here
            if side is not None:
                home = jnp.exp2(local - top)
                share = share + kept_stat[side, pl.ds(2 * tile + 1, 1), :] * home
            if partials:
                there = jnp.exp2(other - top)
                share = share + there
            share = 1.0 / share
            both = mixed * (here * share)
            if side is not None:
                both = both + kept_mix[side, tile] * (home * share)
            if partials:
                sent = pl.ds(rows + tile * TILE, TILE)
                partial = jnp.concatenate([held[head, 0, sent, :].T, turned[head, :, sent]], axis=1)
                both = both + partial.astype(jnp.float32) * (there * share)
            put(head, span, both.astype(jnp.bfloat16))

        return store

    def jobs_of(head, kind, begin_of, end_of, own_end, store):
        jobs = []
        for tile in range(tiles):
            span = pl.ds(tile * TILE, TILE)
            spans = [(begin_of(tile), end_of(tile) - begin_of(tile))]
            end = functools.partial(store, tile)
            jobs.append((head, query_held[head, span, :], query_marks[:, span], kind, spans, own_end, end))
        return jobs

    def at_tile(tile):
        return tile * TILE

    def at_near(tile):
        return rows

    def at_own(tile):
        return 2 * rows

    def past_own(tile):
        return 2 * rows + (tile + 1) * TILE

    early = SPLIT - 2

    @pl.loop(0, HK)
    def _(head):
        turn_values(head, 2 * rows)

    @pl.when(even)
    def _():
        @pl.loop(1, SPLIT)
        def _(step):
            to_core(step, far).wait_recv()
            turn_values(step, 0)

    @pl.when(odd)
    def _():
        @pl.loop(0, HK)
        def _(head):
            to_core(head, near).wait_recv()
            turn_values(head, rows)

    @pl.loop(0, SPLIT + 3)
    def _(count):
        turn = count - 1

        @pl.when(has_next & even & (turn >= 1) & (turn < SPLIT))
        def _():
            for part in range(PARTS):
                query_to_prev(turn, 0, part).wait_recv()
                attend_back(turn, turn, 2 * rows, 0, part)
                slot_to_next(turn, rows, part).start()

            stat_to_next(turn, turn).start()

        @pl.when(has_next & odd & (turn >= 1) & (turn < SPLIT))
        def _():
            for part in range(PARTS):
                query_to_prev(turn, 1, part).wait_recv()
                attend_back(SPLIT + turn, turn, rows, 2 * rows, part)
                slot_to_next(turn, 0, part).start()

            stat_to_next(turn, SPLIT + turn).start()

        for which, begin in ((even, at_own), (odd, at_near)):

            @pl.when(which & (turn <= 0))
            def _():
                jobs = []
                for side in range(2):
                    head = side * SPLIT + early - turn
                    jobs += jobs_of(head, 0, begin, past_own, True, keep(-2 * turn + side))
                run(jobs)

        @pl.when(turn >= 2)
        def _():
            step = turn - 2

            @pl.when(has_prev)
            def _():
                @pl.when(jnp.logical_and(even, step == 0))
                def _():
                    first_newer(0).wait_recv()
                    for part in range(PARTS):
                        relay(step, rows, 0, part).start()

                @pl.when(jnp.logical_and(odd, step == 0))
                def _():
                    first_newer(1).wait_recv()
                    for part in range(PARTS):
                        relay(step, 0, rows, part).start()

                @pl.when(jnp.logical_and(even, step >= 1))
                def _():
                    for part in range(PARTS):
                        slot_to_next(step, rows, part).wait_recv()
                        relay(step, rows, 0, part).start()

                @pl.when(jnp.logical_and(odd, step >= 1))
                def _():
                    for part in range(PARTS):
                        slot_to_next(step, 0, part).wait_recv()
                        relay(step, 0, rows, part).start()

            @pl.loop(0, 2)
            def _(turn_side):
                side = lax.rem(core + turn_side, 2)
                head = side * SPLIT + step

                @pl.when(jnp.logical_and(has_prev, turn_side == 1))
                def _():
                    for part in range(PARTS):
                        relay(step, 0, rows, part).wait_recv()

                @pl.when(even)
                def _():
                    turn_values(head, rows)

                    @pl.when(step == 0)
                    def _():
                        @pl.when(jnp.logical_and(has_prev, turn_side == 0))
                        def _():
                            first_older(0).wait_recv()

                        @pl.when(jnp.logical_and(has_prev, turn_side == 1))
                        def _():
                            first_older(1).wait_recv()

                        turn_values(head, 0)
                        run(jobs_of(head, 1, at_tile, past_own, True, normal(head)))

                    @pl.when(jnp.logical_and(has_prev, step >= 1))
                    def _():
                        stat_to_next(step, head).wait_recv()

                    @pl.when(jnp.logical_and(step >= 1, step < early))
                    def _():
                        run(jobs_of(head, 0, at_near, past_own, True, merged(head, None, True)))

                    @pl.when(step >= early)
                    def _():
                        run(jobs_of(head, 0, at_near, at_own, False, merged(head, 2 * (step - early) + side, True)))

                @pl.when(odd)
                def _():
                    turn_values(head, 0)

                    @pl.when(step < early)
                    def _():
                        kind = jnp.where(step == 0, 1, 0)
                        run(jobs_of(head, kind, at_tile, past_own, True, normal(head)))

                    @pl.when(step >= early)
                    def _():
                        run(jobs_of(head, 0, at_tile, at_near, False, merged(head, 2 * (step - early) + side, False)))

    @pl.when(even)
    def _():
        @pl.loop(0, HK)
        def _(head):
            to_core(head, near).wait_send()

    @pl.when(odd)
    def _():
        @pl.loop(1, SPLIT)
        def _(head):
            to_core(head, far).wait_send()

    @pl.when(has_next)
    def _():
        for side in range(2):
            first_older(side).wait_send()

        @pl.loop(1, SPLIT)
        def _(step):
            for part in range(PARTS):
                slot_to_next(step, 0, part).wait_send()
            stat_to_next(step, step).wait_send()

    @pl.when(has_prev)
    def _():
        @pl.loop(0, SPLIT)
        def _(step):
            for part in range(PARTS):
                relay(step, 0, rows, part).wait_send()

        @pl.when(even)
        def _():
            @pl.loop(1, SPLIT)
            def _(step):
                for side in range(2):
                    for part in range(PARTS):
                        query_to_prev(step, side, part).wait_send()


def on_device(queries, keys, values, doc_lengths):
    rows = keys.shape[0]
    shards = lax.axis_size("cp")
    window = REACH * rows + TILE
    stats = rows // TILE * GROUPS
    dma = pltpu.SemaphoreType.DMA
    return pl.pallas_call(
        functools.partial(kernel, shards),
        out_shape=pltpu.VMEM(queries.shape, queries.dtype),
        in_specs=[
            pl.BlockSpec(memory_space=pltpu.SMEM),
            pl.BlockSpec(memory_space=pl.ANY),
            pl.BlockSpec(memory_space=pl.ANY),
            pl.BlockSpec(memory_space=pl.ANY),
        ],
        out_specs=pl.BlockSpec(memory_space=pltpu.VMEM),
        scratch_shapes=[
            pltpu.VMEM((HK, 2, (REACH + 1) * rows, DH), keys.dtype),
            pltpu.VMEM((HK, rows, WIDTH), queries.dtype),
            pltpu.VMEM((SPLIT, rows, WIDTH), queries.dtype),
            pltpu.VMEM((SPLIT, 2, rows, DH), keys.dtype),
            pltpu.VMEM((SPLIT, stats, TILE), jnp.float32),
            pltpu.VMEM((HK, stats, TILE), jnp.float32),
            pltpu.VMEM((HK, DH, (REACH + 1) * rows), keys.dtype),
            pltpu.VMEM((2, (REACH + 1) * rows, DH), keys.dtype),
            pltpu.VMEM((DH, 2 * rows), keys.dtype),
            pltpu.VMEM((4, window, WIDTH), jnp.float32),
            pltpu.VMEM((4, rows // TILE, DH, WIDTH), jnp.float32),
            pltpu.VMEM((4, 2 * (rows // TILE), WIDTH), jnp.float32),
            dma((HK, 2)),
            dma((HK,)),
            dma((HK,)),
            dma((HK,)),
            dma((HK, PARTS)),
            dma((SPLIT, PARTS)),
            dma((SPLIT, PARTS)),
            dma((SPLIT, PARTS)),
            dma((2,)),
            dma((4,)),
            dma((SPLIT, PARTS)),
            dma((SPLIT, PARTS)),
            dma((SPLIT,)),
            dma((HK,)),
            pltpu.SemaphoreType.REGULAR,
        ],
        compiler_params=pltpu.CompilerParams(
            collective_id=0, has_side_effects=True, vmem_limit_bytes=36 * 1024 * 1024
        ),
    )(*(pltpu.with_memory_space_constraint(x, pltpu.HBM) for x in (doc_lengths, queries, keys, values)))


def solution(mesh):
    return jax.shard_map(
        on_device,
        mesh=mesh,
        in_specs=(P(("grp", "cp"), None), P(("grp", "cp"), None), P(("grp", "cp"), None), P("grp")),
        out_specs=P(("grp", "cp"), None),
        check_vma=False,
    )
```
